256 devices in a mesh: beam: 32 (over y, z), mp: 8 (over x, core).
Axes of the slice: x: 4, y: 4, z: 8, core: 2. Of those that a mesh axis runs over, the one named last changes fastest.
Arguments:
- queries: bfloat16 [512, 8192], P('beam', 'mp'), may hold values from -100 to 100
- fresh_keys: bfloat16 [512, 1024], P('beam', 'mp'), may hold values from -5 to 5
- fresh_values: bfloat16 [512, 1024], P('beam', 'mp'), may hold values from -5 to 5
- key_pool: bfloat16 [2048, 8, 128, 128], P('beam', 'mp'), may hold values from -5 to 5
- value_pool: bfloat16 [2048, 8, 128, 128], P('beam', 'mp'), may hold values from -5 to 5
- page_table: int32 [512, 4], P('beam'), may hold values from 0 to 63, as said below
- lengths: int32 [512], replicated, may hold values from 2 to 511, as said below
- score_weight: bfloat16 [8192], P('mp'), may hold values from -0.0625 to 0.0625
- running_min: float32 [512], P('beam'), may hold values from 0.2 to 0.9
- boundary: int32 [512], P('beam'), may hold values 0 or 1
- parents: int32 [512], replicated, may hold values from 0 to 511, as said below
- homes: int32 [512], replicated, may hold values from 0 to 511, as said below
Outputs:
- attention: bfloat16 [512, 8192], P('beam', 'mp')
- step_score: float32 [512], P('beam')
- child_score: float32 [512], P('beam')
- new_keys: bfloat16 [2048, 8, 128, 128], P('beam', 'mp')
- new_values: bfloat16 [2048, 8, 128, 128], P('beam', 'mp')
The draws below stay inside these ranges and needn't reach their ends.
Inputs may be any that keep to these rules, and one draw needn't show every extreme that they name: `page_table`: the rows of the 16 old beams of one device together name each of that device's 16 * 4 slots once. `lengths`: some old beam that has a new beam descending from it has the largest length. Of the new beams stored on one device of the beam axis (positions homes[c] // 16 equal), at most one of them has its parent on any one device (parents[c] // 16 equal); in every draw some pairs of devices have exactly 1. homes is a permutation of the positions 0 to 511.
All inputs are finite; a program needn't handle non-finite values. No bound on the sum of `boundary` on one device may be relied on, other than what follows from the above.
Results may differ from the reference program's by a relative error of at most 0.0049.
Values may be sent and summed in bfloat16 or wider, within the bound.
A program may use at most 64 MiB of HBM per device.

```python
import math
import jax
import jax.numpy as jnp
from jax import lax

HEADS = 64
KEY_VALUE_HEADS = 8
D_HEAD = 128
PAGE = 128
PAGES = 4
BEAM_DEV = 16
BEAMS = 512
SLOTS = 2048


def layout(key):
    device_list = BEAMS // BEAM_DEV
    per_device = BEAM_DEV * PAGES
    streams = jax.random.split(jax.random.fold_in(key, 11), device_list)
    tables = jax.vmap(lambda k: jax.random.permutation(k, per_device))(streams)
    return tables.reshape(BEAMS, PAGES).astype(jnp.int32)


def kept_beams(key):
    device_list = BEAMS // BEAM_DEV
    span = PAGES * PAGE
    streams = jax.random.split(jax.random.fold_in(key, 23), 7)
    shifts = jax.vmap(lambda k: jax.random.permutation(k, device_list))(jax.random.split(streams[0], device_list))
    column = jnp.arange(BEAM_DEV) % device_list
    source_dev = (jnp.arange(device_list)[:, None] + shifts[:, column]) % device_list
    first = jax.random.randint(streams[1], (device_list, BEAM_DEV), 0, BEAM_DEV)
    second = jax.random.randint(streams[2], (device_list, BEAM_DEV), 0, BEAM_DEV)
    orders = jax.vmap(lambda k: jax.random.permutation(k, BEAM_DEV))(jax.random.split(streams[3], device_list))
    picked = jnp.take_along_axis(orders[source_dev], jnp.minimum(first, second)[:, :, None], axis=2)[:, :, 0]
    by_position = (source_dev * BEAM_DEV + picked).reshape(BEAMS).astype(jnp.int32)
    relabel = jax.random.permutation(streams[4], BEAMS).astype(jnp.int32)
    everyone = jnp.arange(BEAMS, dtype=jnp.int32)
    parents = jnp.zeros((BEAMS,), jnp.int32).at[relabel].set(by_position)
    homes = jnp.zeros((BEAMS,), jnp.int32).at[relabel].set(everyone)
    factor = jax.random.randint(streams[5], (device_list, 1), 1, 5)
    raw = jax.random.randint(streams[6], (device_list, BEAM_DEV), 0, span // 2)
    lengths = (span - 1 - raw * factor // 4).reshape(BEAMS)
    lengths = lengths.at[by_position[::BEAM_DEV]].set(span - 1).astype(jnp.int32)
    return (parents, homes, lengths)


def caches(key):
    pool = jnp.clip(jax.random.normal(jax.random.fold_in(key, 31), (SLOTS, KEY_VALUE_HEADS, PAGE, D_HEAD), jnp.float32), -5.0, 5.0)
    return pool


def draw_page_table(key, part):
    return layout(key)


def draw_parents(key, part):
    return kept_beams(key)[0]


def draw_homes(key, part):
    return kept_beams(key)[1]


def draw_lengths(key, part):
    return kept_beams(key)[2]


def draw_key_pool(key, part):
    return caches(key).astype(jnp.bfloat16)


def draw_queries(key, part):
    shared_query_rows = jnp.clip(jax.random.normal(jax.random.fold_in(key, 41), (BEAMS, HEADS * D_HEAD), jnp.float32), -5.0, 5.0)
    return shared_query_rows.astype(jnp.bfloat16)


def touch_ends(values, stream_key, least, largest):
    spot = [jax.random.randint(jax.random.fold_in(stream_key, axis), (), 0, length) for axis, length in enumerate(values.shape)]
    widest = values.shape.index(max(values.shape))
    next_to = spot[:widest] + [(spot[widest] + 1) % values.shape[widest]] + spot[widest + 1:]
    return values.at[tuple(spot)].set(least).at[tuple(next_to)].set(largest)


def steps_of(stream_key, dims, pieces, smallest, largest):
    factor_of, own = 1.0, jax.random.fold_in(stream_key, 6)
    for dim, blocks in pieces:
        draws = jnp.exp(jax.random.uniform(jax.random.fold_in(own, dim), (blocks,), jnp.float32, smallest / len(pieces), largest / len(pieces)))
        factor_of = factor_of * jnp.repeat(draws, dims[dim] // blocks).reshape([-1 if axis == dim else 1 for axis in range(len(dims))])
    return factor_of


def gaussian(own_key, shape, spread, most, shards=(), kind=jnp.bfloat16):
    result = jax.random.normal(own_key, shape, jnp.float32) * spread
    if len(shards) > 0:
        result = steps_of(own_key, shape, shards, -0.22, 0.18) * result
    return jnp.clip(result, min=-most, max=most).astype(kind)


def setup_inputs(seed: int = 0) -> dict:
    seeds = jax.random.split(jax.random.key(seed), 13)
    return {
        "queries": draw_queries(jax.random.fold_in(seeds[12], 71), 0),
        "fresh_keys": gaussian(seeds[1], (BEAMS, KEY_VALUE_HEADS * D_HEAD), 1.0, 5.0, ((0, 32), (1, 8))),
        "fresh_values": gaussian(seeds[2], (BEAMS, KEY_VALUE_HEADS * D_HEAD), 1.0, 5.0, ((0, 32), (1, 8))),
        "key_pool": draw_key_pool(jax.random.fold_in(seeds[12], 71), 0),
        "value_pool": gaussian(seeds[4], (SLOTS, KEY_VALUE_HEADS, PAGE, D_HEAD), 1.0, 5.0, ((0, 32), (1, 8))),
        "page_table": draw_page_table(jax.random.fold_in(seeds[12], 71), 0),
        "lengths": draw_lengths(jax.random.fold_in(seeds[12], 71), 0),
        "score_weight": gaussian(seeds[7], (HEADS * D_HEAD,), (HEADS * D_HEAD) ** -0.5, 0.0625, ((0, 8),)),
        "running_min": jnp.clip(0.2 + 0.7 * jax.random.uniform(seeds[8], (BEAMS,), jnp.float32) ** steps_of(seeds[8], (BEAMS,), ((0, 32),), -0.2, 0.2), 0.2, 0.9),
        "boundary": touch_ends((jax.random.randint(seeds[9], (BEAMS,), 0, 2) < 1).astype(jnp.int32), jax.random.fold_in(seeds[9], 1), 0, 1),
        "parents": draw_parents(jax.random.fold_in(seeds[12], 71), 0),
        "homes": draw_homes(jax.random.fold_in(seeds[12], 71), 0),
    }


def reference(queries, fresh_keys, fresh_values, key_pool, value_pool, page_table, lengths, score_weight, running_min, boundary, parents, homes):
    beams = queries.shape[0]
    group = HEADS // KEY_VALUE_HEADS
    span = PAGES * PAGE
    scale = 1.0 / math.sqrt(D_HEAD)
    everyone = jnp.arange(beams, dtype=jnp.int32)
    base = everyone // BEAM_DEV * (BEAM_DEV * PAGES)
    slots = (page_table + base[:, None]).astype(jnp.int32)
    last_slot = jnp.take_along_axis(slots, (lengths // PAGE)[:, None].astype(jnp.int32), axis=1)[:, 0]
    offset = lengths % PAGE
    keys_now = key_pool.at[last_slot, :, offset, :].set(fresh_keys.reshape(beams, KEY_VALUE_HEADS, D_HEAD))
    values_now = value_pool.at[last_slot, :, offset, :].set(fresh_values.reshape(beams, KEY_VALUE_HEADS, D_HEAD))
    positions = jnp.arange(span, dtype=jnp.int32)

    def attend(item):
        query, rows, length = item
        key_rows = keys_now[rows].transpose(1, 0, 2, 3).reshape(KEY_VALUE_HEADS, span, D_HEAD)
        value_rows = values_now[rows].transpose(1, 0, 2, 3).reshape(KEY_VALUE_HEADS, span, D_HEAD)
        grouped = query.reshape(KEY_VALUE_HEADS, group, D_HEAD).astype(jnp.float32)
        scores = jnp.einsum('hgd,htd->hgt', grouped, key_rows.astype(jnp.float32)) * scale
        scores = jnp.where((positions <= length)[None, None, :], scores, -jnp.inf)
        weights = jax.nn.softmax(scores, axis=-1).astype(jnp.bfloat16)
        mixed = jnp.einsum('hgt,htd->hgd', weights.astype(jnp.float32), value_rows.astype(jnp.float32))
        return mixed.reshape(HEADS * D_HEAD).astype(jnp.bfloat16)
    attention = lax.map(attend, (queries, slots, lengths))
    flat = attention.astype(jnp.float32)
    sumsq = lax.optimization_barrier(jnp.sum(flat * flat, axis=1))
    dot = lax.optimization_barrier(jnp.sum(flat * score_weight.astype(jnp.float32)[None, :], axis=1))
    step_score = jax.nn.sigmoid(dot * lax.rsqrt(sumsq / (HEADS * D_HEAD) + 1e-06))
    updated = jnp.where(boundary == 1, jnp.minimum(running_min, step_score), running_min)
    order = jnp.zeros((beams,), jnp.int32).at[homes].set(everyone)
    anchor = parents[order]
    child_score = updated[anchor]
    token_grid = jnp.arange(PAGES, dtype=jnp.int32)[:, None] * PAGE + jnp.arange(PAGE, dtype=jnp.int32)[None, :]

    def carry_pages(item):
        rows, length = item
        live = (token_grid <= length)[:, None, :, None]
        zero = jnp.zeros((), keys_now.dtype)
        return (jnp.where(live, keys_now[rows], zero), jnp.where(live, values_now[rows], zero))
    new_keys, new_values = lax.map(carry_pages, (slots[anchor], lengths[anchor]))
    new_keys = new_keys.reshape(beams * PAGES, KEY_VALUE_HEADS, PAGE, D_HEAD)
    new_values = new_values.reshape(beams * PAGES, KEY_VALUE_HEADS, PAGE, D_HEAD)
    return (attention, step_score, child_score, new_keys, new_values)
```

```python
import functools
import math

import jax
import jax.numpy as jnp
from jax import lax
from jax.experimental import pallas as pl
from jax.experimental.pallas import tpu as pltpu
from jax.sharding import PartitionSpec as P

WAIT = 4
Z_SLOTS = 80
Y_SLOTS = 44
Z_BUFS = 8
Y_BUFS = 4
Y_WAIT = 3
RING_Z = 8
RING_Y = 4


def pick(mask, values, axis):
    return jnp.sum(jnp.where(mask, values, 0), axis=axis)


def plan(parents, homes, lengths, page_table, fresh_at, rank):
    beams = parents.shape[0]
    local, pages = page_table.shape
    pool = local * pages
    every = jnp.arange(beams, dtype=jnp.int32)
    q = pick(homes[None, :] == every[:, None], parents[None, :], 1)
    up = pick(q[:, None] == every[None, :], lengths[None, :], 1) // 128 + 1
    src, dst = q // local, every // local
    sy, sz, dy, dz = src // RING_Z, src % RING_Z, dst // RING_Z, dst % RING_Z
    d = (dz - sz) % RING_Z
    sib = q[:, None] == q[None, :]
    far_p = jnp.max(jnp.where(sib & (d < 4)[None, :], d[None, :], 0), axis=1)
    far_m = jnp.max(jnp.where(sib & (d > 4)[None, :], RING_Z - d[None, :], 0), axis=1)
    far_4 = jnp.max(jnp.where(sib & (d == 4)[None, :], 1, 0), axis=1) > 0
    plus4 = far_4 & ((far_p > far_m) | ((far_p == far_m) & (q % 2 == 1)))
    a = jnp.where(plus4, 4, far_p)
    b = jnp.where(far_4 & ~plus4, 4, far_m)
    first = jnp.max(jnp.where(sib & (every[None, :] < every[:, None]), 1, 0), axis=1) == 0
    up_first = jnp.where(first, up, 0)
    goes_p = (d > 0) & ((d < 4) | ((d == 4) & (a == 4)))
    k = jnp.where(goes_p, d, (RING_Z - d) % RING_Z)
    same = src[:, None] == src[None, :]
    order = beams - 1 - q

    def ahead(far):
        key = far * beams + order
        hit = same & (far > 0)[None, :] & (key[None, :] > key[:, None])
        return pick(hit, up_first[None, :], 1)

    pos_p, pos_m = ahead(a), ahead(b)
    devices = jnp.arange(RING_Y * RING_Z, dtype=jnp.int32)
    from_dev = devices[:, None] == src[None, :]
    starts, counts, total = [], [], jnp.int32(0)
    for far, step in ((a, 1), (b, -1)):
        count = [
            pick(from_dev & (far >= j)[None, :], up_first[None, :], 1).reshape(RING_Y, RING_Z)
            for j in range(1, 5)
        ]
        held = [jnp.roll(count[j], step * j, axis=1) for j in range(4)]
        start = [jnp.zeros((RING_Y, RING_Z), jnp.int32)]
        for j in range(1, 4):
            start.append(
                jnp.maximum(
                    start[-1] + held[j - 1], jnp.roll(start[-1], step, axis=1) + WAIT
                )
            )
        for j in range(4):
            total = jnp.maximum(total, jnp.max(jnp.where(held[j] > 0, start[j] + held[j], 0)))
        starts.append(jnp.stack(start).reshape(4, -1))
        counts.append(jnp.stack(held).reshape(4, -1))
    start_all = jnp.concatenate(starts).reshape(-1)
    node = sy * RING_Z + jnp.where(goes_p, dz + RING_Z - 1, dz + 1) % RING_Z
    cell = (jnp.where(goes_p, 0, 4) + k - 1) * (RING_Y * RING_Z) + node
    cells = jnp.arange(start_all.shape[0], dtype=jnp.int32)
    arrive = pick(cell[:, None] == cells[None, :], start_all[None, :], 1)
    arrive = jnp.where(d == 0, -WAIT, arrive + jnp.where(goes_p, pos_p, pos_m))
    turn = (dy - sy) % RING_Y
    ready = (arrive + WAIT) // 2
    lane = jnp.where(turn > 0, (sy * RING_Z + dz) * RING_Y + turn, -1 - every)
    rank_key = ready * beams + every
    same_lane = lane[:, None] == lane[None, :]
    before = same_lane & (rank_key[None, :] < rank_key[:, None])
    queued = pick(before, up[None, :], 1)
    upto = same_lane & (rank_key[None, :] <= rank_key[:, None])
    slot = queued + jnp.max(jnp.where(upto, (ready - queued)[None, :], -(2**20)), axis=1)
    y_total = jnp.max(jnp.where(turn > 0, slot + up, 0))
    fits = (total <= Z_SLOTS) & (y_total <= Y_SLOTS)

    mine = rank * local + jnp.arange(local, dtype=jnp.int32)
    page_ids = jnp.arange(pages, dtype=jnp.int32)
    own_page = pick(
        (q[:, None] == mine[None, :])[:, :, None], page_table[None, :, :], 1
    )
    is_own = src == rank
    live = page_ids[None, :] < up[:, None]
    t = jnp.arange(Z_SLOTS, dtype=jnp.int32)
    tables = []
    row, col = rank // RING_Z, rank % RING_Z
    for side, (far, pos, step) in enumerate(((a, pos_p, 1), (b, pos_m, -1))):
        sends = (is_own & first & (far > 0))[:, None] & live
        at = jnp.where(sends, pos[:, None] + page_ids[None, :], -1)
        table = pick(
            at.reshape(-1)[:, None] == t[None, :], own_page.reshape(-1)[:, None], 0
        )
        behind = row * RING_Z + (col - step) % RING_Z
        for j in range(1, 4):
            lo = lax.dynamic_index_in_dim(starts[side][j], rank, keepdims=False)
            n = lax.dynamic_index_in_dim(counts[side][j], rank, keepdims=False)
            was = lax.dynamic_index_in_dim(starts[side][j - 1], behind, keepdims=False)
            inside = (t >= lo) & (t < lo + n)
            table = jnp.where(inside, pool + side * Z_SLOTS + t - lo + was, table)
        tables.append(table)
    base = jnp.where(goes_p, pool, pool + Z_SLOTS) + arrive
    held_at = jnp.where(
        (d == 0)[:, None], own_page, base[:, None] + page_ids[None, :]
    )
    s = jnp.arange(Y_SLOTS, dtype=jnp.int32)
    for way in (1, 3, 2):
        sends = ((turn == way) & (sy == row) & (dz == col))[:, None] & live
        at = jnp.where(sends, slot[:, None] + page_ids[None, :], -1)
        tables.append(
            pick(at.reshape(-1)[:, None] == s[None, :], held_at.reshape(-1)[:, None], 0)
        )

    def own(x):
        return lax.dynamic_slice_in_dim(x, rank * local, local)

    live_m, turn_m = own(live), own(turn)
    lands = jnp.where(turn_m == 1, 0, jnp.where(turn_m == 3, Y_SLOTS, 2 * Y_SLOTS)) + own(slot)
    in_store = (turn_m == 0)[:, None] & live_m
    in_land = (turn_m > 0)[:, None] & live_m
    tables.append(jnp.where(in_store, own(held_at), 0).reshape(-1))
    tables.append(jnp.where(in_land, lands[:, None] + page_ids[None, :], 0).reshape(-1))
    tables.append(in_land.astype(jnp.int32).reshape(-1))
    tables.extend(fresh_at)
    child_len = own(pick(q[:, None] == every[None, :], lengths[None, :], 1))
    return fits, jnp.concatenate(tables), child_len, own(q)


def fresh_rows(page_table, own_len):
    local, pages = page_table.shape
    slots = jnp.arange(local * pages, dtype=jnp.int32)
    page_ids = jnp.arange(pages, dtype=jnp.int32)
    last = pick(page_ids[None, :] == (own_len // 128)[:, None], page_table, 1)
    hit = last[:, None] == slots[None, :]
    at = pick(hit, (own_len % 128 + 1)[:, None], 0) - 1
    return at, pick(hit, jnp.arange(local, dtype=jnp.int32)[:, None], 0)


def moving(tab, fk, fv, kp, vp, nk, nv, store, land_z, land_y, relay, buf_z, buf_y, *sems):
    send_z, recv_z, send_y, recv_y, recv_r, send_r = sems
    pool = kp.shape[0]
    me = lax.axis_index("beam")
    row, col = me // RING_Z, me % RING_Z
    z_next = row * RING_Z + lax.rem(col + 1, RING_Z)
    z_last = row * RING_Z + lax.rem(col + RING_Z - 1, RING_Z)
    y_next = lax.rem(row + 1, RING_Y) * RING_Z + col
    y_last = lax.rem(row + RING_Y - 1, RING_Y) * RING_Z + col
    z_to, y_to = (z_next, z_last), (y_next, y_last)
    mesh_id = pl.DeviceIdType.MESH

    barrier = pltpu.get_barrier_semaphore()
    for peer in (z_next, z_last, y_next, y_last):
        pl.semaphore_signal(barrier, inc=1, device_id={"beam": peer}, device_id_type=mesh_id)

    y_tab = 2 * Z_SLOTS
    out_tab = y_tab + 3 * Y_SLOTS
    at_tab = out_tab + 3 * pool
    rows = lax.broadcasted_iota(jnp.int32, (128, 128), 0)

    def fill(i, carry):
        at, who = tab[at_tab + i], tab[at_tab + pool + i]
        hit = rows == at
        for half, (new, old) in enumerate(((fk, kp), (fv, vp))):
            line = jnp.broadcast_to(new[who], (128, 128))
            page = jnp.where(hit, line, old[i].astype(jnp.float32))
            store[i, half * 128 : half * 128 + 128] = page.astype(jnp.bfloat16)
        return carry

    lax.fori_loop(0, pool, fill, 0)
    pl.semaphore_wait(barrier, 4)

    def z_copy(side, t, b):
        return pltpu.make_async_remote_copy(
            buf_z.at[side * Z_BUFS + b], land_z.at[side * Z_SLOTS + t],
            send_z.at[side * Z_BUFS + b], recv_z.at[side * Z_SLOTS + t],
            device_id={"beam": z_to[side]}, device_id_type=mesh_id,
        )

    def a_copy(side, s, b):
        return pltpu.make_async_remote_copy(
            buf_y.at[side * Y_BUFS + b], land_y.at[side * Y_SLOTS + s],
            send_y.at[side * Y_BUFS + b], recv_y.at[side * Y_SLOTS + s],
            device_id={"beam": y_to[side]}, device_id_type=mesh_id,
        )

    def d_copy(side, s, b):
        return pltpu.make_async_remote_copy(
            buf_y.at[2 * Y_BUFS + b], relay.at[s],
            send_y.at[2 * Y_BUFS + b], recv_r.at[s],
            device_id={"beam": y_to[side]}, device_id_type=mesh_id,
        )

    def r_copy(side, s):
        return pltpu.make_async_remote_copy(
            relay.at[s], land_y.at[2 * Y_SLOTS + s],
            send_r.at[s], recv_y.at[2 * Y_SLOTS + s],
            device_id={"beam": y_to[side]}, device_id_type=mesh_id,
        )

    def z_slot(g, j):
        t = 4 * g + j

        @pl.when((t >= WAIT) & (t < Z_SLOTS + WAIT))
        def _():
            for side in range(2):
                z_copy(side, t - WAIT, 0).wait_recv()
                at = side * Z_SLOTS + t - WAIT
                store[pool + at] = land_z[at]

        @pl.when(t < Z_SLOTS)
        def _():
            b = lax.rem(g, 2) * 4 + j
            for side in range(2):
                @pl.when(g >= 2)
                def _(side=side):
                    z_copy(side, t - Z_BUFS, b).wait_send()

                buf_z[side * Z_BUFS + b] = store[tab[side * Z_SLOTS + t]]
                z_copy(side, t, b).start()

    def y_slot(g, j):
        s = 2 * g + j

        @pl.when(s < Y_SLOTS)
        def _():
            b = lax.rem(g, 2) * 2 + j

            @pl.when(g >= 2)
            def _():
                a_copy(0, s - Y_BUFS, b).wait_send()
                a_copy(1, s - Y_BUFS, b).wait_send()
                d_copy(j, s - Y_BUFS, b).wait_send()

            for way in range(3):
                buf_y[way * Y_BUFS + b] = store[tab[y_tab + way * Y_SLOTS + s]]
            d_copy(j, s, b).start()
            a_copy(0, s, b).start()
            a_copy(1, s, b).start()

        @pl.when((s >= Y_WAIT) & (s < Y_SLOTS + Y_WAIT))
        def _():
            side = 1 - j if Y_WAIT % 2 else j
            d_copy(side, s - Y_WAIT, 0).wait_recv()
            r_copy(side, s - Y_WAIT).start()

    def group(g, carry):
        z_slot(g, 0)
        z_slot(g, 1)
        y_slot(g, 0)
        z_slot(g, 2)
        z_slot(g, 3)
        y_slot(g, 1)
        return carry

    groups = max(-(-(Z_SLOTS + WAIT) // 4), -(-(Y_SLOTS + Y_WAIT) // 2))
    lax.fori_loop(0, groups, group, 0)

    def drain(i, carry):
        for j in range(2):
            s = 2 * i + j
            a_copy(0, s, 0).wait_recv()
            a_copy(1, s, 0).wait_recv()
            r_copy(j, s).wait_recv()
            r_copy(j, s).wait_send()
        return carry

    lax.fori_loop(0, Y_SLOTS // 2, drain, 0)
    for b in range(Z_BUFS):
        for side in range(2):
            z_copy(side, 0, b).wait_send()
    for b in range(Y_BUFS):
        a_copy(0, 0, b).wait_send()
        a_copy(1, 0, b).wait_send()
        d_copy(b % 2, 0, b).wait_send()

    def finish(i, carry):
        moved = jnp.broadcast_to(tab[out_tab + 2 * pool + i], (128, 128)) > 0
        for half, out in enumerate((nk, nv)):
            part = pl.ds(half * 128, 128)
            here = store[tab[out_tab + i], part].astype(jnp.float32)
            there = land_y[tab[out_tab + pool + i], part].astype(jnp.float32)
            out[i] = jnp.where(moved, there, here).astype(jnp.bfloat16)
        return carry

    lax.fori_loop(0, pool, finish, 0)


def move(tables, fresh_k, fresh_v, keys, values):
    pool = keys.shape[0]
    page = (256, 128)
    out = jax.ShapeDtypeStruct(keys.shape, keys.dtype)
    vmem = pl.BlockSpec(memory_space=pltpu.VMEM)
    dma = pltpu.SemaphoreType.DMA
    return pl.pallas_call(
        moving,
        out_shape=(out, out),
        in_specs=[pl.BlockSpec(memory_space=pltpu.SMEM)] + [vmem] * 4,
        out_specs=(vmem, vmem),
        scratch_shapes=[
            pltpu.VMEM((pool + 2 * Z_SLOTS, *page), jnp.bfloat16),
            pltpu.VMEM((2 * Z_SLOTS, *page), jnp.bfloat16),
            pltpu.VMEM((3 * Y_SLOTS, *page), jnp.bfloat16),
            pltpu.VMEM((Y_SLOTS, *page), jnp.bfloat16),
            pltpu.VMEM((2 * Z_BUFS, *page), jnp.bfloat16),
            pltpu.VMEM((3 * Y_BUFS, *page), jnp.bfloat16),
            dma((2 * Z_BUFS,)),
            dma((2 * Z_SLOTS,)),
            dma((3 * Y_BUFS,)),
            dma((3 * Y_SLOTS,)),
            dma((Y_SLOTS,)),
            dma((Y_SLOTS,)),
        ],
        compiler_params=pltpu.CompilerParams(
            collective_id=0, has_side_effects=True, vmem_limit_bytes=60 * 1024 * 1024
        ),
        name="move_pages",
    )(tables, fresh_k, fresh_v, keys, values)


def sent_to_all(array, axis):
    copies = jnp.broadcast_to(array, (lax.axis_size(axis), *array.shape))
    return lax.all_to_all(copies, axis, split_axis=0, concat_axis=0, tiled=True)


def over_copies(array, axis):
    return sent_to_all(array, axis).sum(axis=0)


def packed_total(arrays, axis):
    ends = [0]
    for a in arrays:
        ends.append(ends[-1] + a.size)
    running = over_copies(jnp.concatenate([a.ravel() for a in arrays]), axis)
    return tuple((running[b:e].reshape(a.shape) for a, b, e in zip(arrays, ends, ends[1:])))


def laid_out(parts, dim):
    parts = jnp.moveaxis(parts, 0, dim)
    dims = parts.shape
    return parts.reshape(*dims[:dim], dims[dim] * dims[dim + 1], *dims[dim + 2 :])


def collect(array, axis, dim):
    return laid_out(sent_to_all(array, axis), dim)


def per_device(
    queries,
    fresh_keys,
    fresh_values,
    key_pool,
    value_pool,
    page_table,
    lengths,
    score_weight,
    running_min,
    boundary,
    parents,
    homes,
):
    ranks = lax.axis_size("beam")
    rank = lax.axis_index("beam")
    local_beams, pages = page_table.shape
    kv_local = key_pool.shape[1]
    page_length = key_pool.shape[2]
    head_dim = key_pool.shape[3]
    heads_local = queries.shape[1] // head_dim
    group = heads_local // kv_local
    beams = lengths.shape[0]
    everyone = jnp.arange(beams, dtype=jnp.int32)
    page_ids = jnp.arange(pages, dtype=jnp.int32)
    token_grid = page_ids[:, None] * page_length + jnp.arange(page_length, dtype=jnp.int32)[None, :]
    own_len = lax.dynamic_slice_in_dim(lengths, rank * local_beams, local_beams)
    last_page = jnp.take_along_axis(page_table, (own_len // page_length)[:, None], axis=1)[:, 0]
    offset_in = own_len % page_length
    keys_now = key_pool.at[last_page, :, offset_in, :].set(
        fresh_keys.reshape(local_beams, kv_local, head_dim)
    )
    values_now = value_pool.at[last_page, :, offset_in, :].set(
        fresh_values.reshape(local_beams, kv_local, head_dim)
    )
    scale = 1.0 / math.sqrt(head_dim)
    key_rows = keys_now[page_table]
    value_rows = values_now[page_table]
    query = queries.reshape(local_beams, kv_local, group, head_dim)
    scores = (
        jnp.einsum("bhgd,bphtd->bhgpt", query, key_rows, preferred_element_type=jnp.float32) * scale
    )
    live_own = (token_grid[None] <= own_len[:, None, None])[:, None, None]
    scores = jnp.where(live_own, scores, -jnp.inf)
    flattened_scores = scores.reshape(local_beams, kv_local, group, pages * page_length)
    weights = jax.nn.softmax(flattened_scores, axis=-1).astype(jnp.bfloat16).reshape(scores.shape)
    mixed = jnp.einsum("bhgpt,bphtd->bhgd", weights, value_rows, preferred_element_type=jnp.float32)
    attention = mixed.reshape(local_beams, heads_local * head_dim).astype(jnp.bfloat16)
    as_float = attention.astype(jnp.float32)
    partial_square = jnp.sum(as_float * as_float, axis=1)
    partial_dot = jnp.sum(as_float * score_weight.astype(jnp.float32)[None, :], axis=1)
    total_square, total_dot = packed_total((partial_square, partial_dot), "mp")
    width = heads_local * head_dim * lax.axis_size("mp")
    step_score = jax.nn.sigmoid(total_dot * lax.rsqrt(total_square / width + 1e-06))
    updated = jnp.where(boundary == 1, jnp.minimum(running_min, step_score), running_min)
    every_updated = collect(updated, "beam", 0)

    def slow():
        capacity = (local_beams + ranks - 1) // ranks
        slot_cap = capacity * pages
        buffer_rows = ranks * slot_cap
        parent_hit = parents[:, None] == everyone[None, :]
        parent_len = jnp.sum(jnp.where(parent_hit, lengths[None, :], 0), axis=1)
        used_pages = parent_len // page_length + 1
        source = parents // local_beams
        destination = homes // local_beams
        earlier = everyone[None, :] < everyone[:, None]
        same_pair = (
            (source[:, None] == source[None, :])
            & (destination[:, None] == destination[None, :])
            & earlier
        )
        offset_table = jnp.sum(jnp.where(same_pair, used_pages[None, :], 0), axis=1)
        sending = (source == rank)[:, None] & (page_ids[None, :] < used_pages[:, None])
        dest_rows = destination[:, None] * slot_cap + offset_table[:, None] + page_ids[None, :]
        dest_rows = jnp.where(sending, dest_rows, buffer_rows)
        local_parent = jnp.clip(parents - rank * local_beams, 0, local_beams - 1)
        source_slots = page_table[local_parent]
        send_table = (
            jnp.zeros((buffer_rows,), jnp.int32)
            .at[dest_rows.reshape(-1)]
            .set(source_slots.reshape(-1), mode="drop")
        )
        positions = rank * local_beams + jnp.arange(local_beams, dtype=jnp.int32)
        child_hit = homes[None, :] == positions[:, None]
        child_source = jnp.sum(jnp.where(child_hit, source[None, :], 0), axis=1)
        child_offset = jnp.sum(jnp.where(child_hit, offset_table[None, :], 0), axis=1)
        child_len = jnp.sum(jnp.where(child_hit, parent_len[None, :], 0), axis=1)
        child_parent = jnp.sum(jnp.where(child_hit, parents[None, :], 0), axis=1)
        recv_rows = jnp.clip(
            child_source[:, None] * slot_cap + child_offset[:, None] + page_ids[None, :],
            0,
            buffer_rows - 1,
        )
        moved_keys, moved_values = (
            lax.all_to_all(keys_now[send_table], "beam", split_axis=0, concat_axis=0, tiled=True),
            lax.all_to_all(values_now[send_table], "beam", split_axis=0, concat_axis=0, tiled=True),
        )
        shape = (local_beams * pages, page_length, head_dim)
        return moved_keys[recv_rows].reshape(shape), moved_values[recv_rows].reshape(shape)

    fits, tables, child_len, child_parent = plan(
        parents, homes, lengths, page_table, fresh_rows(page_table, own_len), rank
    )

    def fast():
        shape = (local_beams * pages, page_length, head_dim)
        return move(
            tables,
            fresh_keys.astype(jnp.float32)[:, None, :],
            fresh_values.astype(jnp.float32)[:, None, :],
            key_pool.reshape(shape),
            value_pool.reshape(shape),
        )

    child_score = jnp.sum(
        jnp.where(child_parent[:, None] == everyone[None, :], every_updated[None, :], 0.0), axis=1
    )
    landed_keys, landed_values = lax.cond(fits, fast, slow)
    live_child = (token_grid[None] <= child_len[:, None, None]).reshape(
        local_beams * pages, 1, page_length, 1
    )
    zero = jnp.zeros((), landed_keys.dtype)
    new_keys = jnp.where(live_child, landed_keys[:, None], zero)
    new_values = jnp.where(live_child, landed_values[:, None], zero)
    return (attention, step_score, child_score, new_keys, new_values)


def solution(mesh):
    in_specs = (
        P("beam", "mp"),
        P("beam", "mp"),
        P("beam", "mp"),
        P("beam", "mp", None, None),
        P("beam", "mp", None, None),
        P("beam", None),
        P(),
        P("mp"),
        P("beam"),
        P("beam"),
        P(),
        P(),
    )
    out_specs = (
        P("beam", "mp"),
        P("beam"),
        P("beam"),
        P("beam", "mp", None, None),
        P("beam", "mp", None, None),
    )
    return jax.shard_map(
        per_device, mesh=mesh, in_specs=in_specs, out_specs=out_specs, check_vma=False
    )
```

```python
import functools
import math

import jax
import jax.numpy as jnp
from jax import lax
from jax.experimental import pallas as pl
from jax.experimental.pallas import tpu as pltpu
from jax.sharding import PartitionSpec as P

WAIT = 4
Y_WAIT = 3
Z_BUFS = 8
Y_BUFS = 4
RING_Z = 8
RING_Y = 4
ROUTES = ((80, 44),)
PAGE = 128
LANES = 128
Z_ROW, Y_ROW, STORE_ROW, LAND_ROW, MOVED_ROW = 0, 2, 5, 6, 7
FRESH_ROW, WHO_ROW, PARENT_ROW, LENGTH_ROW, OWN_ROW = 8, 9, 10, 11, 12
MESH = pl.DeviceIdType.MESH


def planning(parents_ref, homes_ref, lengths_ref, table_ref, tab_ref, need_ref):
    f32 = jnp.float32
    beams = parents_ref.shape[1]
    local, pages = table_ref.shape
    pool = local * pages
    rank = lax.axis_index("beam")
    rank_f = rank.astype(f32)
    row_f, col_f = (rank // RING_Z).astype(f32), (rank % RING_Z).astype(f32)

    def iota(shape, dim):
        return lax.broadcasted_iota(jnp.int32, shape, dim).astype(f32)

    def div(x, n):
        return jnp.floor(x * (1.0 / n))

    def mod(x, n):
        return x - n * div(x, n)

    def columns(*rows):
        packed = jnp.concatenate(
            list(rows) + [jnp.zeros((8 - len(rows), beams), f32)] * (len(rows) < 8), axis=0
        )
        turned = jnp.transpose(packed)
        return [turned[:, i : i + 1] for i in range(len(rows))]

    def add(mask, column):
        return jnp.sum(jnp.where(mask, column, 0.0), axis=0, keepdims=True)

    def top(mask, column, least=0.0):
        return jnp.max(jnp.where(mask, column, least), axis=0, keepdims=True)

    parents, homes, lengths = (
        ref[...].astype(f32) for ref in (parents_ref, homes_ref, lengths_ref)
    )
    parents_c, homes_c, lengths_c = columns(parents, homes, lengths)
    every = iota((1, beams), 1)
    every_c = iota((beams, 1), 0)
    q = add(homes_c == every, parents_c)
    length = add(every_c == q, lengths_c)
    up = div(length, PAGE) + 1.0
    src, dst = div(q, local), div(every, local)
    sy, sz, dy, dz = div(src, RING_Z), mod(src, RING_Z), div(dst, RING_Z), mod(dst, RING_Z)
    d = mod(dz - sz + RING_Z, RING_Z)
    q_c, up_c, d_c = columns(q, up, d)
    src_c = div(q_c, local)
    sib = q_c == q
    far_p = top(sib, jnp.where(d_c < 4, d_c, 0.0))
    far_m = top(sib, jnp.where(d_c > 4, RING_Z - d_c, 0.0))
    far_4 = top(sib, jnp.where(d_c == 4, 1.0, 0.0)) > 0
    first = top(sib & (every_c < every), 1.0) == 0
    plus4 = far_4 & ((far_p > far_m) | ((far_p == far_m) & (mod(q, 2) == 1)))
    a = jnp.where(plus4, 4.0, far_p)
    b = jnp.where(far_4 & jnp.logical_not(plus4), 4.0, far_m)
    up_first = jnp.where(first, up, 0.0)
    goes_p = (d > 0) & ((d < 4) | ((d == 4) & (a == 4)))
    k = jnp.where(goes_p, d, mod(RING_Z - d, RING_Z))
    a_c, b_c, upf_c = columns(a, b, up_first)
    same = src_c == src
    order, order_c = beams - 1 - q, beams - 1 - q_c
    pos_p = add(
        same & (a_c * beams + order_c > a * beams + order), jnp.where(a_c > 0, upf_c, 0.0)
    )
    pos_m = add(
        same & (b_c * beams + order_c > b * beams + order), jnp.where(b_c > 0, upf_c, 0.0)
    )

    weights = jnp.concatenate(
        [jnp.where(far >= j, up_first, 0.0) for far in (a, b) for j in range(1, 5)], axis=0
    )
    lane = iota((1, LANES), 1)
    count = jnp.dot(weights, jnp.where(src_c == lane, 1.0, 0.0), preferred_element_type=f32)
    at_z = mod(lane, RING_Z)

    def back(x, n):
        n = n % RING_Z
        if n == 0:
            return x
        full = jnp.broadcast_to(x, (8, LANES))
        near = pltpu.roll(full, n, 1)
        wrap = pltpu.roll(full, LANES + n - RING_Z, 1)
        return jnp.where(at_z >= n, near, wrap)[:1]

    starts, helds, total = [], [], jnp.zeros((1, LANES), f32)
    for side in range(2):
        step = 1 - 2 * side
        held = [back(count[4 * side + j : 4 * side + j + 1], step * j) for j in range(4)]
        start = [jnp.zeros((1, LANES), f32)]
        for j in range(1, 4):
            start.append(jnp.maximum(start[-1] + held[j - 1], back(start[-1], step) + WAIT))
        for j in range(4):
            total = jnp.maximum(total, jnp.where(held[j] > 0, start[j] + held[j], 0.0))
        starts.append(start)
        helds.append(held)
    z_total = jnp.max(total)
    node = sy * RING_Z + mod(jnp.where(goes_p, dz + RING_Z - 1, dz + 1), RING_Z)
    spots = jnp.where(iota((LANES, 1), 0) == node, 1.0, 0.0)
    seen = jnp.dot(
        jnp.concatenate(starts[0] + starts[1], axis=0), spots,
        preferred_element_type=f32, precision=lax.Precision.HIGHEST,
    )
    seen = jnp.floor(seen + 0.5)
    cell = jnp.where(goes_p, 0.0, 4.0) + k - 1
    arrive = jnp.zeros((1, beams), f32)
    for j in range(8):
        arrive = jnp.where(cell == j, seen[j : j + 1], arrive)
    arrive = jnp.where(d == 0, -1.0 * WAIT, arrive + jnp.where(goes_p, pos_p, pos_m))
    turn = mod(dy - sy + RING_Y, RING_Y)
    ready = div(arrive + WAIT, 2)
    queue = jnp.where(turn > 0, (sy * RING_Z + dz) * RING_Y + turn, -1 - every)
    rank_key = ready * beams + every
    queue_c, rank_c, ready_c, pos_p_c, pos_m_c, arrive_c, turn_c, goes_c = columns(
        queue, rank_key, ready, pos_p, pos_m, arrive, turn, jnp.where(goes_p, 1.0, 0.0)
    )
    same_queue = queue_c == queue
    queued = add(same_queue & (rank_c < rank_key), up_c)
    (queued_c,) = columns(queued)
    slot = queued + top(same_queue & (rank_c <= rank_key), ready_c - queued_c, -1e6)
    y_total = jnp.max(jnp.where(turn > 0, slot + up, 0.0))
    need_ref[0] = z_total.astype(jnp.int32)
    need_ref[1] = y_total.astype(jnp.int32)

    (slot_c,) = columns(slot)
    table = table_ref[...].astype(f32)
    mine = jnp.where(q_c == rank_f * local + iota((1, local), 1), 1.0, 0.0)
    own_page = jnp.dot(mine, table, preferred_element_type=f32)
    own_c = [own_page[:, p : p + 1] for p in range(pages)]
    first_c = upf_c > 0
    is_own_c = src_c == rank_f
    tables = []
    for side, (far_c, pos_c) in enumerate(((a_c, pos_p_c), (b_c, pos_m_c))):
        step = 1 - 2 * side
        sends = is_own_c & first_c & (far_c > 0)
        line = jnp.zeros((1, LANES), f32)
        for p in range(pages):
            at = jnp.where(sends & (up_c > p), pos_c + p, -1.0)
            line += add(at == lane, own_c[p])
        for j in range(1, 4):
            pick = lambda x: jnp.sum(jnp.where(lane == rank_f, x, 0.0), axis=1, keepdims=True)
            lo, n = pick(starts[side][j]), pick(helds[side][j])
            was = pick(back(starts[side][j - 1], step))
            line = jnp.where(
                (lane >= lo) & (lane < lo + n), pool + side + 2 * (lane - lo + was), line
            )
        tables.append(line)
    here_c = d_c == 0
    base_c = jnp.where(goes_c > 0, pool * 1.0, pool + 1.0) + 2 * arrive_c
    held_c = [jnp.where(here_c, own_c[p], base_c + 2 * p) for p in range(pages)]
    sy_c = div(src_c, RING_Z)
    dz_c = mod(div(every_c, local), RING_Z)
    at_me = (sy_c == row_f) & (dz_c == col_f)
    for way in (1.0, 3.0, 2.0):
        line = jnp.zeros((1, LANES), f32)
        for p in range(pages):
            at = jnp.where(at_me & (turn_c == way) & (up_c > p), slot_c + p, -1.0)
            line += add(at == lane, held_c[p])
        tables.append(line)
    way_c = jnp.where(turn_c == 1, 0.0, jnp.where(turn_c == 3, 1.0, 2.0))
    child = every_c == rank_f * local + div(lane, pages)
    from_store, from_land, moved = [jnp.zeros((1, LANES), f32)] * 3
    for p in range(pages):
        hit = child & (mod(lane, pages) == p) & (lane < pool) & (up_c > p)
        from_store += add(hit & (turn_c == 0), held_c[p])
        from_land += add(hit & (turn_c > 0), 3 * (slot_c + p) + way_c)
        moved += add(hit & (turn_c > 0), 1.0)
    tables += [from_store, from_land, moved]
    owner = rank_f * local + iota((local, 1), 0)
    own_len = jnp.sum(jnp.where(every == owner, lengths, 0.0), axis=1, keepdims=True)
    fresh, who = jnp.zeros((1, LANES), f32), jnp.zeros((1, LANES), f32)
    for p in range(pages):
        hit = (table[:, p : p + 1] == lane) & (div(own_len, PAGE) == p)
        fresh += add(hit, mod(own_len, PAGE) + 1)
        who += add(hit, iota((local, 1), 0))
    length_c = jnp.sum(jnp.where(q_c == every, lengths, 0.0), axis=1, keepdims=True)
    mine_lane = (every_c == rank_f * local + lane) & (lane < local)
    tables += [fresh - 1, who, add(mine_lane, q_c), add(mine_lane, length_c)]
    tables.append(add(mine_lane, lengths_c))
    tables += [jnp.zeros((1, LANES), f32)] * (16 - len(tables))
    tab_ref[...] = jnp.concatenate(tables, axis=0).astype(jnp.int32)


def plan(parents, homes, lengths, page_table):
    vmem = pl.BlockSpec(memory_space=pltpu.VMEM)
    return pl.pallas_call(
        planning,
        out_shape=(
            jax.ShapeDtypeStruct((16, LANES), jnp.int32),
            jax.ShapeDtypeStruct((2,), jnp.int32),
        ),
        in_specs=[vmem] * 4,
        out_specs=(vmem, pl.BlockSpec(memory_space=pltpu.SMEM)),
        name="plan_moves",
    )(parents[None], homes[None], lengths[None], page_table)


def moving(z_slots, y_slots, *refs):
    tab, pages_of, least, ends, fk, fv, q_ref, sw, kp, vp, att, score, nk, nv = refs[:14]
    store, land_z, land_y, relay, buf_z, buf_y, sums, land_s, land_u = refs[14:23]
    send_z, recv_z, send_y, recv_y, recv_r, send_r, send_s, recv_s, send_u, recv_u = refs[23:]
    pool = kp.shape[0]
    local, heads, head_dim = q_ref.shape
    pages = pool // local
    f32 = jnp.float32
    me, part = lax.axis_index("beam"), lax.axis_index("mp")
    parts = lax.axis_size("mp")
    row, col = me // RING_Z, me % RING_Z

    def at_z(n):
        return row * RING_Z + lax.rem(col + n, RING_Z)

    def at_y(n):
        return lax.rem(row + n, RING_Y) * RING_Z + col

    z_to, y_to = (at_z(1), at_z(RING_Z - 1)), (at_y(1), at_y(RING_Y - 1))
    barrier = pltpu.get_barrier_semaphore()

    def greet(where):
        pl.semaphore_signal(barrier, inc=1, device_id=where, device_id_type=MESH)

    for n in range(1, RING_Z):
        greet({"beam": at_z(n)})
    for n in range(1, RING_Y):
        greet({"beam": at_y(n)})
    for n in range(1, parts):
        greet({"mp": lax.rem(part + n, parts)})

    rows = lax.broadcasted_iota(jnp.int32, (PAGE, head_dim), 0)

    def fill(i, carry):
        hit = rows == tab[FRESH_ROW, i]
        who = tab[WHO_ROW, i]
        for half, (new, old) in enumerate(((fk, kp), (fv, vp))):
            line = jnp.broadcast_to(new[who], (PAGE, head_dim))
            page = jnp.where(hit, line, old[i].astype(f32))
            store[i, half * PAGE : half * PAGE + PAGE] = page.astype(jnp.bfloat16)
        return carry

    lax.fori_loop(0, pool, fill, 0)
    pl.semaphore_wait(barrier, RING_Z + RING_Y + parts - 3)

    def remote(source, target, sent, got, where):
        return pltpu.make_async_remote_copy(
            source, target, sent, got, device_id=where, device_id_type=MESH
        )

    def z_copy(side, t, b):
        b = side * Z_BUFS + b
        return remote(
            buf_z.at[b], land_z.at[2 * t + side], send_z.at[b], recv_z.at[2 * t + side],
            {"beam": z_to[side]},
        )

    def a_copy(side, s, b):
        b = side * Y_BUFS + b
        return remote(
            buf_y.at[b], land_y.at[3 * s + side], send_y.at[b], recv_y.at[3 * s + side],
            {"beam": y_to[side]},
        )

    def d_copy(side, s, b):
        b = 2 * Y_BUFS + b
        return remote(buf_y.at[b], relay.at[s], send_y.at[b], recv_r.at[s], {"beam": y_to[side]})

    def r_copy(side, s):
        return remote(
            relay.at[s], land_y.at[3 * s + 2], send_r.at[s], recv_y.at[3 * s + 2],
            {"beam": y_to[side]},
        )

    def s_copy(n, origin):
        return remote(
            sums, land_s.at[origin], send_s.at[n], recv_s.at[origin],
            {"mp": lax.rem(part + n, parts)},
        )

    def u_copy(n, origin):
        spot = land_u.at[row, origin]
        return remote(spot, spot, send_u.at[n], recv_u.at[origin], {"beam": at_z(n)})

    def v_copy(n, origin):
        spot = land_u.at[origin]
        return remote(
            spot, spot, send_u.at[RING_Z + n], recv_u.at[RING_Z + origin], {"beam": at_y(n)}
        )

    def z_slot(g, j):
        t = 4 * g + j

        @pl.when((t >= WAIT) & (t < z_slots + WAIT))
        def _():
            for side in range(2):
                z_copy(side, t - WAIT, 0).wait_recv()
                at = 2 * (t - WAIT) + side
                store[pool + at] = land_z[at]

        @pl.when(t < z_slots)
        def _():
            b = lax.rem(g, 2) * 4 + j
            for side in range(2):

                @pl.when(g >= 2)
                def _(side=side):
                    z_copy(side, t - Z_BUFS, b).wait_send()

                buf_z[side * Z_BUFS + b] = store[tab[Z_ROW + side, t]]
                z_copy(side, t, b).start()

    def y_slot(g, j):
        s = 2 * g + j

        @pl.when(s < y_slots)
        def _():
            b = lax.rem(g, 2) * 2 + j

            @pl.when(g >= 2)
            def _():
                a_copy(0, s - Y_BUFS, b).wait_send()
                a_copy(1, s - Y_BUFS, b).wait_send()
                d_copy(j, s - Y_BUFS, b).wait_send()

            for way in range(3):
                buf_y[way * Y_BUFS + b] = store[tab[Y_ROW + way, s]]
            d_copy(j, s, b).start()
            a_copy(0, s, b).start()
            a_copy(1, s, b).start()

        @pl.when((s >= Y_WAIT) & (s < y_slots + Y_WAIT))
        def _():
            side = 1 - j if Y_WAIT % 2 else j
            d_copy(side, s - Y_WAIT, 0).wait_recv()
            r_copy(side, s - Y_WAIT).start()

    def attend(i):
        keys = jnp.concatenate([store[pages_of[i, p], :PAGE] for p in range(pages)], axis=0)
        logits = lax.dot_general(
            q_ref[i], keys, (((1,), (1,)), ((), ())), preferred_element_type=f32
        ) * (1.0 / math.sqrt(head_dim))
        token = lax.broadcasted_iota(jnp.int32, logits.shape, 1)
        logits = jnp.where(token <= tab[OWN_ROW, i], logits, -jnp.inf)
        powers = jnp.exp(logits - jnp.max(logits, axis=1, keepdims=True))
        weights = (powers / jnp.sum(powers, axis=1, keepdims=True)).astype(jnp.bfloat16)
        values = jnp.concatenate([store[pages_of[i, p], PAGE:] for p in range(pages)], axis=0)
        mixed = jnp.dot(weights, values, preferred_element_type=f32).astype(jnp.bfloat16)
        att[i] = mixed
        mixed = mixed.astype(f32)
        for n, other in enumerate((mixed, sw[...].astype(f32))):
            total = jnp.sum(jnp.sum(mixed * other, axis=1, keepdims=True), axis=0, keepdims=True)
            sums[n, i] = jnp.broadcast_to(total, (1, LANES))

    lane = lax.broadcasted_iota(jnp.int32, (1, LANES), 1)

    def tell_sums():
        land_s[part] = sums[...]
        for n in range(1, parts):
            s_copy(n, part).start()

    def tell_updated():
        for n in range(1, parts):
            s_copy(n, lax.rem(part + parts - n, parts)).wait_recv()
        both = land_s[0]
        for n in range(1, parts):
            both += land_s[n]
        updated = jnp.zeros((1, LANES), f32)
        steps = jnp.zeros((1, LANES), f32)
        for i in range(local):
            width = heads * head_dim * parts
            step = jax.nn.sigmoid(both[1, i] * lax.rsqrt(both[0, i] / width + 1e-06))
            floor = jnp.broadcast_to(least[i], (1, LANES))
            ended = jnp.broadcast_to(ends[i], (1, LANES)) == 1
            new = jnp.where(ended, jnp.minimum(floor, step), floor)
            steps = jnp.where(lane == i, step, steps)
            updated = jnp.where(lane == i, new, updated)
        score[0:1, :] = steps
        land_u[row, col] = updated
        for n in range(1, RING_Z):
            u_copy(n, col).start()

    def tell_row():
        for n in range(1, RING_Z):
            u_copy(n, lax.rem(col + RING_Z - n, RING_Z)).wait_recv()
        for n in range(1, RING_Y):
            v_copy(n, row).start()

    def give_children():
        for n in range(1, RING_Y):
            v_copy(n, lax.rem(row + RING_Y - n, RING_Y)).wait_recv()
        out = jnp.zeros((1, LANES), f32)
        for i in range(local):
            q = tab[PARENT_ROW, i]
            line = land_u[q // (local * RING_Z), (q // local) % RING_Z]
            value = jnp.sum(jnp.where(lane == q % local, line, 0.0), axis=1, keepdims=True)
            out = jnp.where(lane == i, jnp.broadcast_to(value, (1, LANES)), out)
        score[1:2, :] = out
        for n in range(1, parts):
            s_copy(n, part).wait_send()
        for n in range(1, RING_Z):
            u_copy(n, col).wait_send()
        for n in range(1, RING_Y):
            v_copy(n, row).wait_send()

    def group(g, carry):
        z_slot(g, 0)
        z_slot(g, 1)
        y_slot(g, 0)

        @pl.when(g < local)
        def _():
            attend(g)

        z_slot(g, 2)
        z_slot(g, 3)
        y_slot(g, 1)
        for n, act in enumerate((tell_sums, tell_updated, tell_row, give_children)):
            pl.when(g == local + (0, 1, 2, 3)[n])(act)
        return carry

    groups = max(-(-(z_slots + WAIT) // 4), -(-(y_slots + Y_WAIT) // 2))
    lax.fori_loop(0, groups, group, 0)

    def drain(i, carry):
        for j in range(2):
            s = 2 * i + j
            a_copy(0, s, 0).wait_recv()
            a_copy(1, s, 0).wait_recv()
            r_copy(j, s).wait_recv()
            r_copy(j, s).wait_send()
        return carry

    lax.fori_loop(0, y_slots // 2, drain, 0)
    for b in range(Z_BUFS):
        for side in range(2):
            z_copy(side, 0, b).wait_send()
    for b in range(Y_BUFS):
        a_copy(0, 0, b).wait_send()
        a_copy(1, 0, b).wait_send()
        d_copy(b % 2, 0, b).wait_send()

    def finish(i, carry):
        moved = jnp.broadcast_to(tab[MOVED_ROW, i], (PAGE, head_dim)) > 0
        live = rows + lax.rem(i, pages) * PAGE <= tab[LENGTH_ROW, i // pages]
        for half, out in enumerate((nk, nv)):
            side = pl.ds(half * PAGE, PAGE)
            here = store[tab[STORE_ROW, i], side].astype(f32)
            there = land_y[tab[LAND_ROW, i], side].astype(f32)
            page = jnp.where(live, jnp.where(moved, there, here), 0.0)
            out[i] = page.astype(jnp.bfloat16)
        return carry

    lax.fori_loop(0, pool, finish, 0)


def move(z_slots, y_slots, tables, page_table, running_min, boundary, fresh_k, fresh_v, query,
         score_weight, keys, values):
    pool = keys.shape[0]
    page = (2 * PAGE, keys.shape[2])
    out = jax.ShapeDtypeStruct(keys.shape, keys.dtype)
    vmem, smem = pl.BlockSpec(memory_space=pltpu.VMEM), pl.BlockSpec(memory_space=pltpu.SMEM)
    dma = pltpu.SemaphoreType.DMA
    parts = lax.axis_size("mp")
    local = query.shape[0]
    return pl.pallas_call(
        functools.partial(moving, z_slots, y_slots),
        out_shape=(
            jax.ShapeDtypeStruct(query.shape, query.dtype),
            jax.ShapeDtypeStruct((2, LANES), jnp.float32),
            out,
            out,
        ),
        in_specs=[smem] * 4 + [vmem] * 6,
        out_specs=(vmem,) * 4,
        scratch_shapes=[
            pltpu.VMEM((pool + 2 * z_slots, *page), jnp.bfloat16),
            pltpu.VMEM((2 * z_slots, *page), jnp.bfloat16),
            pltpu.VMEM((3 * y_slots, *page), jnp.bfloat16),
            pltpu.VMEM((y_slots, *page), jnp.bfloat16),
            pltpu.VMEM((2 * Z_BUFS, *page), jnp.bfloat16),
            pltpu.VMEM((3 * Y_BUFS, *page), jnp.bfloat16),
            pltpu.VMEM((2, local, 1, LANES), jnp.float32),
            pltpu.VMEM((parts, 2, local, 1, LANES), jnp.float32),
            pltpu.VMEM((RING_Y, RING_Z, 1, LANES), jnp.float32),
            dma((2 * Z_BUFS,)),
            dma((2 * z_slots,)),
            dma((3 * Y_BUFS,)),
            dma((3 * y_slots,)),
            dma((y_slots,)),
            dma((y_slots,)),
            dma((parts,)),
            dma((parts,)),
            dma((RING_Z + RING_Y,)),
            dma((RING_Z + RING_Y,)),
        ],
        compiler_params=pltpu.CompilerParams(
            collective_id=0, has_side_effects=True, vmem_limit_bytes=60 * 1024 * 1024
        ),
        name="move_pages",
    )(tables, page_table, running_min, boundary, fresh_k, fresh_v, query, score_weight, keys, values)


def sent_to_all(array, axis):
    copies = jnp.broadcast_to(array, (lax.axis_size(axis), *array.shape))
    return lax.all_to_all(copies, axis, split_axis=0, concat_axis=0, tiled=True)


def over_copies(array, axis):
    return sent_to_all(array, axis).sum(axis=0)


def packed_total(arrays, axis):
    ends = [0]
    for a in arrays:
        ends.append(ends[-1] + a.size)
    running = over_copies(jnp.concatenate([a.ravel() for a in arrays]), axis)
    return tuple((running[b:e].reshape(a.shape) for a, b, e in zip(arrays, ends, ends[1:])))


def laid_out(parts, dim):
    parts = jnp.moveaxis(parts, 0, dim)
    dims = parts.shape
    return parts.reshape(*dims[:dim], dims[dim] * dims[dim + 1], *dims[dim + 2 :])


def collect(array, axis, dim):
    return laid_out(sent_to_all(array, axis), dim)


def whole_exchange(
    queries,
    fresh_keys,
    fresh_values,
    key_pool,
    value_pool,
    page_table,
    lengths,
    score_weight,
    running_min,
    boundary,
    parents,
    homes,
):
    ranks = lax.axis_size("beam")
    rank = lax.axis_index("beam")
    local_beams, pages = page_table.shape
    kv_local = key_pool.shape[1]
    page_length = key_pool.shape[2]
    head_dim = key_pool.shape[3]
    heads_local = queries.shape[1] // head_dim
    group = heads_local // kv_local
    beams = lengths.shape[0]
    capacity = (local_beams + ranks - 1) // ranks
    slot_cap = capacity * pages
    buffer_rows = ranks * slot_cap
    everyone = jnp.arange(beams, dtype=jnp.int32)
    page_ids = jnp.arange(pages, dtype=jnp.int32)
    token_grid = page_ids[:, None] * page_length + jnp.arange(page_length, dtype=jnp.int32)[None, :]
    parent_hit = parents[:, None] == everyone[None, :]
    parent_len = jnp.sum(jnp.where(parent_hit, lengths[None, :], 0), axis=1)
    used_pages = parent_len // page_length + 1
    source = parents // local_beams
    destination = homes // local_beams
    earlier = everyone[None, :] < everyone[:, None]
    same_pair = (
        (source[:, None] == source[None, :])
        & (destination[:, None] == destination[None, :])
        & earlier
    )
    offset_table = jnp.sum(jnp.where(same_pair, used_pages[None, :], 0), axis=1)
    sending = (source == rank)[:, None] & (page_ids[None, :] < used_pages[:, None])
    dest_rows = destination[:, None] * slot_cap + offset_table[:, None] + page_ids[None, :]
    dest_rows = jnp.where(sending, dest_rows, buffer_rows)
    local_parent = jnp.clip(parents - rank * local_beams, 0, local_beams - 1)
    source_slots = page_table[local_parent]
    send_table = (
        jnp.zeros((buffer_rows,), jnp.int32)
        .at[dest_rows.reshape(-1)]
        .set(source_slots.reshape(-1), mode="drop")
    )
    positions = rank * local_beams + jnp.arange(local_beams, dtype=jnp.int32)
    child_hit = homes[None, :] == positions[:, None]
    child_source = jnp.sum(jnp.where(child_hit, source[None, :], 0), axis=1)
    child_offset = jnp.sum(jnp.where(child_hit, offset_table[None, :], 0), axis=1)
    child_len = jnp.sum(jnp.where(child_hit, parent_len[None, :], 0), axis=1)
    child_parent = jnp.sum(jnp.where(child_hit, parents[None, :], 0), axis=1)
    recv_rows = jnp.clip(
        child_source[:, None] * slot_cap + child_offset[:, None] + page_ids[None, :],
        0,
        buffer_rows - 1,
    )
    own_len = lax.dynamic_slice_in_dim(lengths, rank * local_beams, local_beams)
    last_page = jnp.take_along_axis(page_table, (own_len // page_length)[:, None], axis=1)[:, 0]
    offset_in = own_len % page_length
    keys_now = key_pool.at[last_page, :, offset_in, :].set(
        fresh_keys.reshape(local_beams, kv_local, head_dim)
    )
    values_now = value_pool.at[last_page, :, offset_in, :].set(
        fresh_values.reshape(local_beams, kv_local, head_dim)
    )
    scale = 1.0 / math.sqrt(head_dim)
    key_rows = keys_now[page_table]
    value_rows = values_now[page_table]
    query = queries.reshape(local_beams, kv_local, group, head_dim)
    scores = (
        jnp.einsum("bhgd,bphtd->bhgpt", query, key_rows, preferred_element_type=jnp.float32) * scale
    )
    live_own = (token_grid[None] <= own_len[:, None, None])[:, None, None]
    scores = jnp.where(live_own, scores, -jnp.inf)
    flattened_scores = scores.reshape(local_beams, kv_local, group, pages * page_length)
    weights = jax.nn.softmax(flattened_scores, axis=-1).astype(jnp.bfloat16).reshape(scores.shape)
    mixed = jnp.einsum("bhgpt,bphtd->bhgd", weights, value_rows, preferred_element_type=jnp.float32)
    attention = mixed.reshape(local_beams, heads_local * head_dim).astype(jnp.bfloat16)
    as_float = attention.astype(jnp.float32)
    partial_square = jnp.sum(as_float * as_float, axis=1)
    partial_dot = jnp.sum(as_float * score_weight.astype(jnp.float32)[None, :], axis=1)
    total_square, total_dot = packed_total((partial_square, partial_dot), "mp")
    width = heads_local * head_dim * lax.axis_size("mp")
    step_score = jax.nn.sigmoid(total_dot * lax.rsqrt(total_square / width + 1e-06))
    updated = jnp.where(boundary == 1, jnp.minimum(running_min, step_score), running_min)
    every_updated = collect(updated, "beam", 0)
    child_score = jnp.sum(
        jnp.where(child_parent[:, None] == everyone[None, :], every_updated[None, :], 0.0), axis=1
    )
    moved_keys, moved_values = (
        lax.all_to_all(keys_now[send_table], "beam", split_axis=0, concat_axis=0, tiled=True),
        lax.all_to_all(values_now[send_table], "beam", split_axis=0, concat_axis=0, tiled=True),
    )
    landed_keys = moved_keys[recv_rows]
    landed_values = moved_values[recv_rows]
    live_child = (token_grid[None] <= child_len[:, None, None])[:, :, None, :, None]
    zero = jnp.zeros((), landed_keys.dtype)
    new_keys = jnp.where(live_child, landed_keys, zero).reshape(
        local_beams * pages, kv_local, page_length, head_dim
    )
    new_values = jnp.where(live_child, landed_values, zero).reshape(
        local_beams * pages, kv_local, page_length, head_dim
    )
    return (attention, step_score, child_score, new_keys, new_values)


def per_device(*args):
    (queries, fresh_keys, fresh_values, key_pool, value_pool, page_table) = args[:6]
    (lengths, score_weight, running_min, boundary, parents, homes) = args[6:]
    local = queries.shape[0]
    pool, kv, page, head_dim = key_pool.shape
    tables, need = plan(parents, homes, lengths, page_table)
    route = jnp.int32(len(ROUTES))
    for n, (z_slots, y_slots) in reversed(tuple(enumerate(ROUTES))):
        route = jnp.where((need[0] <= z_slots) & (need[1] <= y_slots), n, route)

    def streamed(z_slots, y_slots):
        attention, score, new_keys, new_values = move(
            z_slots,
            y_slots,
            tables,
            page_table,
            running_min,
            boundary,
            fresh_keys.astype(jnp.float32)[:, None, :],
            fresh_values.astype(jnp.float32)[:, None, :],
            queries.reshape(local, -1, head_dim),
            score_weight.reshape(-1, head_dim),
            key_pool.reshape(pool, page, head_dim),
            value_pool.reshape(pool, page, head_dim),
        )
        return (
            attention.reshape(queries.shape),
            score[0, :local],
            score[1, :local],
            new_keys.reshape(key_pool.shape),
            new_values.reshape(value_pool.shape),
        )

    ways = [functools.partial(streamed, *r) for r in ROUTES]
    return lax.switch(route, ways + [lambda: whole_exchange(*args)])


def solution(mesh):
    in_specs = (
        P("beam", "mp"),
        P("beam", "mp"),
        P("beam", "mp"),
        P("beam", "mp", None, None),
        P("beam", "mp", None, None),
        P("beam", None),
        P(),
        P("mp"),
        P("beam"),
        P("beam"),
        P(),
        P(),
    )
    out_specs = (
        P("beam", "mp"),
        P("beam"),
        P("beam"),
        P("beam", "mp", None, None),
        P("beam", "mp", None, None),
    )
    return jax.shard_map(
        per_device, mesh=mesh, in_specs=in_specs, out_specs=out_specs, check_vma=False
    )
```

```python
import functools
import math

import jax
import jax.numpy as jnp
from jax import lax
from jax.experimental import pallas as pl
from jax.experimental.pallas import tpu as pltpu
from jax.sharding import PartitionSpec as P

WAIT = 4
Y_WAIT = 3
Z_BUFS = 8
Y_BUFS = 4
RING_Z = 8
RING_Y = 4
ROUTES = ((72, 38, 36), (80, 44, 42))
ROUNDS = 2
VMEM_BYTES = 49 * 1024 * 1024
PAGE = 128
LANES = 128
Z_ROW, Y_ROW, STORE_ROW, LAND_ROW, MOVED_ROW = 0, 2, 5, 6, 7
FRESH_ROW, WHO_ROW, PARENT_ROW, LENGTH_ROW, OWN_ROW = 8, 9, 10, 11, 12
PAGE_ROW = 13
MESH = pl.DeviceIdType.MESH


def planning(parents_ref, homes_ref, lengths_ref, table_ref, tab_ref, need_ref):
    f32 = jnp.float32
    beams = parents_ref.shape[1]
    local, pages = table_ref.shape
    pool = local * pages
    rank = lax.axis_index("beam")
    rank_f = rank.astype(f32)
    row_f, col_f = (rank // RING_Z).astype(f32), (rank % RING_Z).astype(f32)

    def iota(shape, dim):
        return lax.broadcasted_iota(jnp.int32, shape, dim).astype(f32)

    def div(x, n):
        return jnp.floor(x * (1.0 / n))

    def mod(x, n):
        return x - n * div(x, n)

    def columns(*rows):
        packed = jnp.concatenate(
            list(rows) + [jnp.zeros((8 - len(rows), beams), f32)] * (len(rows) < 8), axis=0
        )
        turned = jnp.transpose(packed)
        return [turned[:, i : i + 1] for i in range(len(rows))]

    def add(mask, column):
        return jnp.sum(jnp.where(mask, column, 0.0), axis=0, keepdims=True)

    def top(mask, column, least=0.0):
        return jnp.max(jnp.where(mask, column, least), axis=0, keepdims=True)

    parents, homes, lengths = (
        ref[...].astype(f32) for ref in (parents_ref, homes_ref, lengths_ref)
    )
    parents_c, homes_c, lengths_c = columns(parents, homes, lengths)
    every = iota((1, beams), 1)
    every_c = iota((beams, 1), 0)
    q = add(homes_c == every, parents_c)
    length = add(every_c == q, lengths_c)
    up = div(length, PAGE) + 1.0
    src, dst = div(q, local), div(every, local)
    sy, sz, dy, dz = div(src, RING_Z), mod(src, RING_Z), div(dst, RING_Z), mod(dst, RING_Z)
    d = mod(dz - sz + RING_Z, RING_Z)
    q_c, up_c, d_c = columns(q, up, d)
    src_c = div(q_c, local)
    sib = q_c == q
    far_p = top(sib, jnp.where(d_c < 4, d_c, 0.0))
    far_m = top(sib, jnp.where(d_c > 4, RING_Z - d_c, 0.0))
    far_4 = top(sib, jnp.where(d_c == 4, 1.0, 0.0)) > 0
    first = top(sib & (every_c < every), 1.0) == 0
    plus4 = far_4 & ((far_p > far_m) | ((far_p == far_m) & (mod(q, 2) == 1)))
    up_first = jnp.where(first, up, 0.0)
    lane = iota((1, LANES), 1)
    at_z = mod(lane, RING_Z)
    from_node = jnp.where(src_c == lane, 1.0, 0.0)
    at_node = jnp.where(iota((LANES, 1), 0) == src, 1.0, 0.0)

    def back(x, n):
        n = n % RING_Z
        if n == 0:
            return x
        full = jnp.broadcast_to(x, (8, LANES))
        near = pltpu.roll(full, n, 1)
        wrap = pltpu.roll(full, LANES + n - RING_Z, 1)
        return jnp.where(at_z >= n, near, wrap)[:1]

    def reach(plus):
        plus = jnp.where(plus, 1.0, 0.0)
        split = jnp.where(far_4, 1.0, 0.0)
        a = jnp.maximum(far_p, 4.0 * split * plus)
        b = jnp.maximum(far_m, 4.0 * split * (1.0 - plus))
        weights = jnp.concatenate(
            [jnp.where(far >= j, up_first, 0.0) for far in (a, b) for j in range(1, 5)], axis=0
        )
        count = jnp.dot(weights, from_node, preferred_element_type=f32)
        held = [
            [back(count[4 * n + j : 4 * n + j + 1], (1 - 2 * n) * j) for j in range(4)]
            for n in range(2)
        ]
        return a, b, held

    for turn in range(ROUNDS):
        a, b, helds = reach(plus4)
        loads = [sum(held) for held in helds]
        ahead = [back(loads[n], (2 * n - 1) * j) for n in range(2) for j in range(4)]
        seen = jnp.dot(jnp.concatenate(ahead, axis=0), at_node, preferred_element_type=f32)
        plus = jnp.where(plus4, 1.0, 0.0)
        cost_p, cost_m = jnp.zeros((1, beams), f32), jnp.zeros((1, beams), f32)
        for j in range(4):
            over_p = jnp.maximum(seen[j : j + 1] + up * (1 - plus) - 30, 0.0)
            over_m = jnp.maximum(seen[4 + j : 5 + j] + up * plus - 30, 0.0)
            cost_p += jnp.where(far_p <= j, over_p * over_p, 0.0)
            cost_m += jnp.where(far_m <= j, over_m * over_m, 0.0)
        moves = mod(q + src, ROUNDS) == turn
        want = jnp.where(cost_p < cost_m, 1.0, 0.0)
        plus4 = jnp.where(moves, want, plus) > 0
    a, b, helds = reach(plus4)
    goes_p = (d > 0) & ((d < 4) | ((d == 4) & (a == 4)))
    k = jnp.where(goes_p, d, mod(RING_Z - d, RING_Z))
    a_c, b_c, upf_c = columns(a, b, up_first)
    same = src_c == src
    order, order_c = beams - 1 - q, beams - 1 - q_c
    pos_p = add(
        same & (a_c * beams + order_c > a * beams + order), jnp.where(a_c > 0, upf_c, 0.0)
    )
    pos_m = add(
        same & (b_c * beams + order_c > b * beams + order), jnp.where(b_c > 0, upf_c, 0.0)
    )

    starts, total = [], jnp.zeros((1, LANES), f32)
    for side in range(2):
        step = 1 - 2 * side
        held = helds[side]
        start = [jnp.zeros((1, LANES), f32)]
        for j in range(1, 4):
            start.append(jnp.maximum(start[-1] + held[j - 1], back(start[-1], step) + WAIT))
        for j in range(4):
            total = jnp.maximum(total, jnp.where(held[j] > 0, start[j] + held[j], 0.0))
        starts.append(start)
    z_total = jnp.max(total)
    node = sy * RING_Z + mod(jnp.where(goes_p, dz + RING_Z - 1, dz + 1), RING_Z)
    spots = jnp.where(iota((LANES, 1), 0) == node, 1.0, 0.0)
    seen = jnp.dot(
        jnp.concatenate(starts[0] + starts[1], axis=0), spots,
        preferred_element_type=f32, precision=lax.Precision.HIGHEST,
    )
    seen = jnp.floor(seen + 0.5)
    cell = jnp.where(goes_p, 0.0, 4.0) + k - 1
    arrive = jnp.zeros((1, beams), f32)
    for j in range(8):
        arrive = jnp.where(cell == j, seen[j : j + 1], arrive)
    arrive = jnp.where(d == 0, -1.0 * WAIT, arrive + jnp.where(goes_p, pos_p, pos_m))
    turn = mod(dy - sy + RING_Y, RING_Y)
    ready = div(arrive + WAIT, 2)
    queue = jnp.where(turn > 0, (sy * RING_Z + dz) * RING_Y + turn, -1 - every)
    rank_key = ready * beams + every
    queue_c, rank_c, ready_c, pos_p_c, pos_m_c, arrive_c, turn_c, goes_c = columns(
        queue, rank_key, ready, pos_p, pos_m, arrive, turn, jnp.where(goes_p, 1.0, 0.0)
    )
    same_queue = queue_c == queue
    queued = add(same_queue & (rank_c < rank_key), up_c)
    (queued_c,) = columns(queued)
    slot = queued + top(same_queue & (rank_c <= rank_key), ready_c - queued_c, -1e6)
    ends = slot + up
    a_total = jnp.max(jnp.where((turn == 1) | (turn == 3), ends, 0.0))
    d_total = jnp.max(jnp.where(turn == 2, ends, 0.0))
    route = jnp.float32(len(ROUTES))
    for n in reversed(range(len(ROUTES))):
        z_slots, y_slots, d_slots = ROUTES[n]
        fits = (z_total <= z_slots) & (a_total <= y_slots) & (d_total <= d_slots)
        route = jnp.where(fits, jnp.float32(n), route)
    need_ref[0] = route.astype(jnp.int32)

    (slot_c,) = columns(slot)
    table = table_ref[...].astype(f32)
    mine = jnp.where(q_c == rank_f * local + iota((1, local), 1), 1.0, 0.0)
    own_page = jnp.dot(mine, table, preferred_element_type=f32)
    own_c = [own_page[:, p : p + 1] for p in range(pages)]
    first_c = upf_c > 0
    is_own_c = src_c == rank_f
    tables = []
    for side, (far_c, pos_c) in enumerate(((a_c, pos_p_c), (b_c, pos_m_c))):
        step = 1 - 2 * side
        sends = is_own_c & first_c & (far_c > 0)
        line = jnp.zeros((1, LANES), f32)
        for p in range(pages):
            at = jnp.where(sends & (up_c > p), pos_c + p, -1.0)
            line += add(at == lane, own_c[p])
        for j in range(1, 4):
            pick = lambda x: jnp.sum(jnp.where(lane == rank_f, x, 0.0), axis=1, keepdims=True)
            lo, n = pick(starts[side][j]), pick(helds[side][j])
            was = pick(back(starts[side][j - 1], step))
            line = jnp.where(
                (lane >= lo) & (lane < lo + n), pool + side + 2 * (lane - lo + was), line
            )
        tables.append(line)
    here_c = d_c == 0
    base_c = jnp.where(goes_c > 0, pool * 1.0, pool + 1.0) + 2 * arrive_c
    held_c = [jnp.where(here_c, own_c[p], base_c + 2 * p) for p in range(pages)]
    sy_c = div(src_c, RING_Z)
    dz_c = mod(div(every_c, local), RING_Z)
    at_me = (sy_c == row_f) & (dz_c == col_f)
    for way in (1.0, 3.0, 2.0):
        line = jnp.zeros((1, LANES), f32)
        for p in range(pages):
            at = jnp.where(at_me & (turn_c == way) & (up_c > p), slot_c + p, -1.0)
            line += add(at == lane, held_c[p])
        tables.append(line)
    way_c = jnp.where(turn_c == 1, 0.0, jnp.where(turn_c == 3, 1.0, 2.0))
    child = every_c == rank_f * local + div(lane, pages)
    from_store, from_land, moved = [jnp.zeros((1, LANES), f32)] * 3
    for p in range(pages):
        hit = child & (mod(lane, pages) == p) & (lane < pool) & (up_c > p)
        from_store += add(hit & (turn_c == 0), held_c[p])
        from_land += add(hit & (turn_c > 0), 3 * (slot_c + p) + way_c)
        moved += add(hit & (turn_c > 0), 1.0)
    tables += [from_store, from_land, moved]
    owner = rank_f * local + iota((local, 1), 0)
    own_len = jnp.sum(jnp.where(every == owner, lengths, 0.0), axis=1, keepdims=True)
    fresh, who = jnp.zeros((1, LANES), f32), jnp.zeros((1, LANES), f32)
    for p in range(pages):
        hit = (table[:, p : p + 1] == lane) & (div(own_len, PAGE) == p)
        fresh += add(hit, mod(own_len, PAGE) + 1)
        who += add(hit, iota((local, 1), 0))
    length_c = jnp.sum(jnp.where(q_c == every, lengths, 0.0), axis=1, keepdims=True)
    mine_lane = (every_c == rank_f * local + lane) & (lane < local)
    tables += [fresh - 1, who, add(mine_lane, q_c), add(mine_lane, length_c)]
    tables.append(add(mine_lane, lengths_c))
    at_beam = iota((local, 1), 0) == div(lane, pages)
    tables.append(
        sum(add(at_beam & (mod(lane, pages) == p), table[:, p : p + 1]) for p in range(pages))
    )
    tables += [jnp.zeros((1, LANES), f32)] * (16 - len(tables))
    tab_ref[...] = jnp.concatenate(tables, axis=0).astype(jnp.int32)


def plan(parents, homes, lengths, page_table):
    vmem = pl.BlockSpec(memory_space=pltpu.VMEM)
    return pl.pallas_call(
        planning,
        out_shape=(
            jax.ShapeDtypeStruct((16, LANES), jnp.int32),
            jax.ShapeDtypeStruct((1,), jnp.int32),
        ),
        in_specs=[vmem] * 4,
        out_specs=(vmem, pl.BlockSpec(memory_space=pltpu.SMEM)),
        name="plan_moves",
    )(parents[None], homes[None], lengths[None], page_table)


def moving(z_slots, y_slots, d_slots, *refs):
    tab, least, ends, fk, fv, q_ref, sw, kp, vp, att, score, nk, nv = refs[:13]
    store, land_z, land_y, relay, buf_z, buf_y, sums, land_s, land_u, fresh = refs[13:23]
    send_z, recv_z, send_y, recv_y, recv_r, send_r, send_s, recv_s, send_u, recv_u = refs[23:]
    pool = kp.shape[0]
    local, heads, head_dim = q_ref.shape
    pages = pool // local
    f32 = jnp.float32
    me, part = lax.axis_index("beam"), lax.axis_index("mp")
    parts = lax.axis_size("mp")
    row, col = me // RING_Z, me % RING_Z

    def at_z(n):
        return row * RING_Z + lax.rem(col + n, RING_Z)

    def at_y(n):
        return lax.rem(row + n, RING_Y) * RING_Z + col

    z_to, y_to = (at_z(1), at_z(RING_Z - 1)), (at_y(1), at_y(RING_Y - 1))
    barrier = pltpu.get_barrier_semaphore()

    def greet(where):
        pl.semaphore_signal(barrier, inc=1, device_id=where, device_id_type=MESH)

    for n in range(1, RING_Z):
        greet({"beam": at_z(n)})
    for n in range(1, RING_Y):
        greet({"beam": at_y(n)})
    for n in range(1, parts):
        greet({"mp": lax.rem(part + n, parts)})

    rows = lax.broadcasted_iota(jnp.int32, (PAGE, head_dim), 0)
    for n, new in enumerate((fk, fv)):
        lines = new[...].astype(f32)
        for i in range(local):
            fresh[n, i] = lines[i : i + 1]

    def fill(i, carry):
        hit = rows == tab[FRESH_ROW, i]
        who = tab[WHO_ROW, i]
        for half, old in enumerate((kp, vp)):
            line = jnp.broadcast_to(fresh[half, who], (PAGE, head_dim))
            page = jnp.where(hit, line, old[i].astype(f32))
            store[i, half * PAGE : half * PAGE + PAGE] = page.astype(jnp.bfloat16)
        return carry

    lax.fori_loop(0, pool, fill, 0, unroll=4)
    pl.semaphore_wait(barrier, RING_Z + RING_Y + parts - 3)

    def remote(source, target, sent, got, where):
        return pltpu.make_async_remote_copy(
            source, target, sent, got, device_id=where, device_id_type=MESH
        )

    def z_copy(side, t, b):
        b = side * Z_BUFS + b
        return remote(
            buf_z.at[b], land_z.at[2 * t + side], send_z.at[b], recv_z.at[2 * t + side],
            {"beam": z_to[side]},
        )

    def a_copy(side, s, b):
        b = side * Y_BUFS + b
        return remote(
            buf_y.at[b], land_y.at[3 * s + side], send_y.at[b], recv_y.at[3 * s + side],
            {"beam": y_to[side]},
        )

    def d_copy(side, s, b):
        b = 2 * Y_BUFS + b
        return remote(buf_y.at[b], relay.at[s], send_y.at[b], recv_r.at[s], {"beam": y_to[side]})

    def r_copy(side, s):
        return remote(
            relay.at[s], land_y.at[3 * s + 2], send_r.at[s], recv_y.at[3 * s + 2],
            {"beam": y_to[side]},
        )

    def s_copy(n, origin):
        return remote(
            sums, land_s.at[origin], send_s.at[n], recv_s.at[origin],
            {"mp": lax.rem(part + n, parts)},
        )

    def u_copy(n, origin):
        spot = land_u.at[row, origin]
        return remote(spot, spot, send_u.at[n], recv_u.at[origin], {"beam": at_z(n)})

    def v_copy(n, origin):
        spot = land_u.at[origin]
        return remote(
            spot, spot, send_u.at[RING_Z + n], recv_u.at[RING_Z + origin], {"beam": at_y(n)}
        )

    def z_slot(g, j):
        t = 4 * g + j

        @pl.when((t >= WAIT) & (t < z_slots + WAIT))
        def _():
            for side in range(2):
                z_copy(side, t - WAIT, 0).wait_recv()
                at = 2 * (t - WAIT) + side
                store[pool + at] = land_z[at]

        @pl.when(t < z_slots)
        def _():
            b = lax.rem(g, 2) * 4 + j
            for side in range(2):

                @pl.when(g >= 2)
                def _(side=side):
                    z_copy(side, t - Z_BUFS, b).wait_send()

                buf_z[side * Z_BUFS + b] = store[tab[Z_ROW + side, t]]
                z_copy(side, t, b).start()

    def y_slot(g, j):
        s = 2 * g + j

        @pl.when(s < d_slots)
        def _():
            b = lax.rem(g, 2) * 2 + j

            @pl.when(g >= 2)
            def _():
                d_copy(j, s - Y_BUFS, b).wait_send()

            buf_y[2 * Y_BUFS + b] = store[tab[Y_ROW + 2, s]]
            d_copy(j, s, b).start()

        @pl.when(s < y_slots)
        def _():
            b = lax.rem(g, 2) * 2 + j

            @pl.when(g >= 2)
            def _():
                a_copy(0, s - Y_BUFS, b).wait_send()
                a_copy(1, s - Y_BUFS, b).wait_send()

            for way in range(2):
                buf_y[way * Y_BUFS + b] = store[tab[Y_ROW + way, s]]
            a_copy(0, s, b).start()
            a_copy(1, s, b).start()

        @pl.when((s >= Y_WAIT) & (s < d_slots + Y_WAIT))
        def _():
            side = 1 - j if Y_WAIT % 2 else j
            d_copy(side, s - Y_WAIT, 0).wait_recv()
            r_copy(side, s - Y_WAIT).start()

    def attend(i):
        keys = jnp.concatenate([store[tab[PAGE_ROW, pages * i + p], :PAGE] for p in range(pages)], axis=0)
        logits = lax.dot_general(
            q_ref[i], keys, (((1,), (1,)), ((), ())), preferred_element_type=f32
        ) * (1.0 / math.sqrt(head_dim))
        token = lax.broadcasted_iota(jnp.int32, logits.shape, 1)
        logits = jnp.where(token <= tab[OWN_ROW, i], logits, -jnp.inf)
        powers = jnp.exp(logits - jnp.max(logits, axis=1, keepdims=True))
        weights = (powers / jnp.sum(powers, axis=1, keepdims=True)).astype(jnp.bfloat16)
        values = jnp.concatenate([store[tab[PAGE_ROW, pages * i + p], PAGE:] for p in range(pages)], axis=0)
        mixed = jnp.dot(weights, values, preferred_element_type=f32).astype(jnp.bfloat16)
        att[i] = mixed
        mixed = mixed.astype(f32)
        for n, other in enumerate((mixed, sw[...].astype(f32))):
            total = jnp.sum(jnp.sum(mixed * other, axis=1, keepdims=True), axis=0, keepdims=True)
            sums[n, i] = jnp.broadcast_to(total, (1, LANES))

    lane = lax.broadcasted_iota(jnp.int32, (1, LANES), 1)

    def tell_sums():
        land_s[part] = sums[...]
        for n in range(1, parts):
            s_copy(n, part).start()

    def tell_updated():
        for n in range(1, parts):
            s_copy(n, lax.rem(part + parts - n, parts)).wait_recv()
        both = land_s[0]
        for n in range(1, parts):
            both += land_s[n]
        updated = jnp.zeros((1, LANES), f32)
        steps = jnp.zeros((1, LANES), f32)
        for i in range(local):
            width = heads * head_dim * parts
            step = jax.nn.sigmoid(both[1, i] * lax.rsqrt(both[0, i] / width + 1e-06))
            floor = jnp.broadcast_to(least[i], (1, LANES))
            ended = jnp.broadcast_to(ends[i], (1, LANES)) == 1
            new = jnp.where(ended, jnp.minimum(floor, step), floor)
            steps = jnp.where(lane == i, step, steps)
            updated = jnp.where(lane == i, new, updated)
        score[0:1, :] = steps
        land_u[row, col] = updated
        for n in range(1, RING_Z):
            u_copy(n, col).start()

    def tell_row():
        for n in range(1, RING_Z):
            u_copy(n, lax.rem(col + RING_Z - n, RING_Z)).wait_recv()
        for n in range(1, RING_Y):
            v_copy(n, row).start()

    def give_children():
        for n in range(1, RING_Y):
            v_copy(n, lax.rem(row + RING_Y - n, RING_Y)).wait_recv()
        out = jnp.zeros((1, LANES), f32)
        for i in range(local):
            q = tab[PARENT_ROW, i]
            line = land_u[q // (local * RING_Z), (q // local) % RING_Z]
            value = jnp.sum(jnp.where(lane == q % local, line, 0.0), axis=1, keepdims=True)
            out = jnp.where(lane == i, jnp.broadcast_to(value, (1, LANES)), out)
        score[1:2, :] = out
        for n in range(1, parts):
            s_copy(n, part).wait_send()
        for n in range(1, RING_Z):
            u_copy(n, col).wait_send()
        for n in range(1, RING_Y):
            v_copy(n, row).wait_send()

    def group(g, carry):
        z_slot(g, 0)
        z_slot(g, 1)
        y_slot(g, 0)

        @pl.when(g < local)
        def _():
            attend(g)

        z_slot(g, 2)
        z_slot(g, 3)
        y_slot(g, 1)
        for n, act in enumerate((tell_sums, tell_updated, tell_row, give_children)):
            pl.when(g == local + (0, 1, 2, 3)[n])(act)
        return carry

    groups = max(-(-(z_slots + WAIT) // 4), -(-max(y_slots, d_slots + Y_WAIT) // 2))
    lax.fori_loop(0, groups, group, 0)

    def drain(i, carry):
        for j in range(2):
            s = 2 * i + j
            a_copy(0, s, 0).wait_recv()
            a_copy(1, s, 0).wait_recv()
        return carry

    def drain_d(i, carry):
        for j in range(2):
            s = 2 * i + j
            r_copy(j, s).wait_recv()
            r_copy(j, s).wait_send()
        return carry

    lax.fori_loop(0, y_slots // 2, drain, 0)
    lax.fori_loop(0, d_slots // 2, drain_d, 0)
    for b in range(Z_BUFS):
        for side in range(2):
            z_copy(side, 0, b).wait_send()
    for b in range(Y_BUFS):
        a_copy(0, 0, b).wait_send()
        a_copy(1, 0, b).wait_send()
        d_copy(b % 2, 0, b).wait_send()

    def finish(i, carry):
        moved = jnp.broadcast_to(tab[MOVED_ROW, i], (PAGE, head_dim)) > 0
        live = rows + lax.rem(i, pages) * PAGE <= tab[LENGTH_ROW, i // pages]
        for half, out in enumerate((nk, nv)):
            side = pl.ds(half * PAGE, PAGE)
            here = store[tab[STORE_ROW, i], side].astype(f32)
            there = land_y[tab[LAND_ROW, i], side].astype(f32)
            page = jnp.where(live, jnp.where(moved, there, here), 0.0)
            out[i] = page.astype(jnp.bfloat16)
        return carry

    lax.fori_loop(0, pool, finish, 0, unroll=4)


def move(z_slots, y_slots, d_slots, tables, running_min, boundary, fresh_k, fresh_v, query,
         score_weight, keys, values):
    pool = keys.shape[0]
    page = (2 * PAGE, keys.shape[2])
    out = jax.ShapeDtypeStruct(keys.shape, keys.dtype)
    vmem, smem = pl.BlockSpec(memory_space=pltpu.VMEM), pl.BlockSpec(memory_space=pltpu.SMEM)
    dma = pltpu.SemaphoreType.DMA
    parts = lax.axis_size("mp")
    local = query.shape[0]
    return pl.pallas_call(
        functools.partial(moving, z_slots, y_slots, d_slots),
        out_shape=(
            jax.ShapeDtypeStruct(query.shape, query.dtype),
            jax.ShapeDtypeStruct((2, LANES), jnp.float32),
            out,
            out,
        ),
        in_specs=[smem] * 3 + [vmem] * 6,
        out_specs=(vmem,) * 4,
        scratch_shapes=[
            pltpu.VMEM((pool + 2 * z_slots, *page), jnp.bfloat16),
            pltpu.VMEM((2 * z_slots, *page), jnp.bfloat16),
            pltpu.VMEM((3 * y_slots, *page), jnp.bfloat16),
            pltpu.VMEM((d_slots, *page), jnp.bfloat16),
            pltpu.VMEM((2 * Z_BUFS, *page), jnp.bfloat16),
            pltpu.VMEM((3 * Y_BUFS, *page), jnp.bfloat16),
            pltpu.VMEM((2, local, 1, LANES), jnp.float32),
            pltpu.VMEM((parts, 2, local, 1, LANES), jnp.float32),
            pltpu.VMEM((RING_Y, RING_Z, 1, LANES), jnp.float32),
            pltpu.VMEM((2, local, 1, keys.shape[2]), jnp.float32),
            dma((2 * Z_BUFS,)),
            dma((2 * z_slots,)),
            dma((3 * Y_BUFS,)),
            dma((3 * y_slots,)),
            dma((d_slots,)),
            dma((d_slots,)),
            dma((parts,)),
            dma((parts,)),
            dma((RING_Z + RING_Y,)),
            dma((RING_Z + RING_Y,)),
        ],
        compiler_params=pltpu.CompilerParams(
            collective_id=ROUTES.index((z_slots, y_slots, d_slots)),
            has_side_effects=True,
            vmem_limit_bytes=VMEM_BYTES,
        ),
        name="move_pages",
    )(tables, running_min, boundary, fresh_k, fresh_v, query, score_weight, keys, values)


def sent_to_all(array, axis):
    copies = jnp.broadcast_to(array, (lax.axis_size(axis), *array.shape))
    return lax.all_to_all(copies, axis, split_axis=0, concat_axis=0, tiled=True)


def over_copies(array, axis):
    return sent_to_all(array, axis).sum(axis=0)


def packed_total(arrays, axis):
    ends = [0]
    for a in arrays:
        ends.append(ends[-1] + a.size)
    running = over_copies(jnp.concatenate([a.ravel() for a in arrays]), axis)
    return tuple((running[b:e].reshape(a.shape) for a, b, e in zip(arrays, ends, ends[1:])))


def laid_out(parts, dim):
    parts = jnp.moveaxis(parts, 0, dim)
    dims = parts.shape
    return parts.reshape(*dims[:dim], dims[dim] * dims[dim + 1], *dims[dim + 2 :])


def collect(array, axis, dim):
    return laid_out(sent_to_all(array, axis), dim)


def whole_exchange(
    queries,
    fresh_keys,
    fresh_values,
    key_pool,
    value_pool,
    page_table,
    lengths,
    score_weight,
    running_min,
    boundary,
    parents,
    homes,
):
    ranks = lax.axis_size("beam")
    rank = lax.axis_index("beam")
    local_beams, pages = page_table.shape
    kv_local = key_pool.shape[1]
    page_length = key_pool.shape[2]
    head_dim = key_pool.shape[3]
    heads_local = queries.shape[1] // head_dim
    group = heads_local // kv_local
    beams = lengths.shape[0]
    capacity = (local_beams + ranks - 1) // ranks
    slot_cap = capacity * pages
    buffer_rows = ranks * slot_cap
    everyone = jnp.arange(beams, dtype=jnp.int32)
    page_ids = jnp.arange(pages, dtype=jnp.int32)
    token_grid = page_ids[:, None] * page_length + jnp.arange(page_length, dtype=jnp.int32)[None, :]
    parent_hit = parents[:, None] == everyone[None, :]
    parent_len = jnp.sum(jnp.where(parent_hit, lengths[None, :], 0), axis=1)
    used_pages = parent_len // page_length + 1
    source = parents // local_beams
    destination = homes // local_beams
    earlier = everyone[None, :] < everyone[:, None]
    same_pair = (
        (source[:, None] == source[None, :])
        & (destination[:, None] == destination[None, :])
        & earlier
    )
    offset_table = jnp.sum(jnp.where(same_pair, used_pages[None, :], 0), axis=1)
    sending = (source == rank)[:, None] & (page_ids[None, :] < used_pages[:, None])
    dest_rows = destination[:, None] * slot_cap + offset_table[:, None] + page_ids[None, :]
    dest_rows = jnp.where(sending, dest_rows, buffer_rows)
    local_parent = jnp.clip(parents - rank * local_beams, 0, local_beams - 1)
    source_slots = page_table[local_parent]
    send_table = (
        jnp.zeros((buffer_rows,), jnp.int32)
        .at[dest_rows.reshape(-1)]
        .set(source_slots.reshape(-1), mode="drop")
    )
    positions = rank * local_beams + jnp.arange(local_beams, dtype=jnp.int32)
    child_hit = homes[None, :] == positions[:, None]
    child_source = jnp.sum(jnp.where(child_hit, source[None, :], 0), axis=1)
    child_offset = jnp.sum(jnp.where(child_hit, offset_table[None, :], 0), axis=1)
    child_len = jnp.sum(jnp.where(child_hit, parent_len[None, :], 0), axis=1)
    child_parent = jnp.sum(jnp.where(child_hit, parents[None, :], 0), axis=1)
    recv_rows = jnp.clip(
        child_source[:, None] * slot_cap + child_offset[:, None] + page_ids[None, :],
        0,
        buffer_rows - 1,
    )
    own_len = lax.dynamic_slice_in_dim(lengths, rank * local_beams, local_beams)
    last_page = jnp.take_along_axis(page_table, (own_len // page_length)[:, None], axis=1)[:, 0]
    offset_in = own_len % page_length
    slot_ids = jnp.arange(key_pool.shape[0], dtype=jnp.int32)
    hit = last_page[None, :] == slot_ids[:, None]
    writer = jnp.sum(jnp.where(hit, jnp.arange(local_beams, dtype=jnp.int32), 0), axis=1)
    at = jnp.sum(jnp.where(hit, offset_in[None, :] + 1, 0), axis=1) - 1
    written = (at[:, None] == jnp.arange(page_length, dtype=jnp.int32))[:, None, :, None]

    def with_fresh(fresh, old):
        rows = fresh.reshape(local_beams, kv_local, 1, head_dim)[writer]
        return jnp.where(written, rows, old)

    keys_now = with_fresh(fresh_keys, key_pool)
    values_now = with_fresh(fresh_values, value_pool)
    scale = 1.0 / math.sqrt(head_dim)
    key_rows = keys_now[page_table]
    value_rows = values_now[page_table]
    query = queries.reshape(local_beams, kv_local, group, head_dim)
    scores = (
        jnp.einsum("bhgd,bphtd->bhgpt", query, key_rows, preferred_element_type=jnp.float32) * scale
    )
    live_own = (token_grid[None] <= own_len[:, None, None])[:, None, None]
    scores = jnp.where(live_own, scores, -jnp.inf)
    flattened_scores = scores.reshape(local_beams, kv_local, group, pages * page_length)
    weights = jax.nn.softmax(flattened_scores, axis=-1).astype(jnp.bfloat16).reshape(scores.shape)
    mixed = jnp.einsum("bhgpt,bphtd->bhgd", weights, value_rows, preferred_element_type=jnp.float32)
    attention = mixed.reshape(local_beams, heads_local * head_dim).astype(jnp.bfloat16)
    as_float = attention.astype(jnp.float32)
    partial_square = jnp.sum(as_float * as_float, axis=1)
    partial_dot = jnp.sum(as_float * score_weight.astype(jnp.float32)[None, :], axis=1)
    total_square, total_dot = packed_total((partial_square, partial_dot), "mp")
    width = heads_local * head_dim * lax.axis_size("mp")
    step_score = jax.nn.sigmoid(total_dot * lax.rsqrt(total_square / width + 1e-06))
    updated = jnp.where(boundary == 1, jnp.minimum(running_min, step_score), running_min)
    every_updated = collect(updated, "beam", 0)
    child_score = jnp.sum(
        jnp.where(child_parent[:, None] == everyone[None, :], every_updated[None, :], 0.0), axis=1
    )
    moved_keys, moved_values = (
        lax.all_to_all(keys_now[send_table], "beam", split_axis=0, concat_axis=0, tiled=True),
        lax.all_to_all(values_now[send_table], "beam", split_axis=0, concat_axis=0, tiled=True),
    )
    landed_keys = moved_keys[recv_rows]
    landed_values = moved_values[recv_rows]
    live_child = (token_grid[None] <= child_len[:, None, None])[:, :, None, :, None]
    zero = jnp.zeros((), landed_keys.dtype)
    new_keys = jnp.where(live_child, landed_keys, zero).reshape(
        local_beams * pages, kv_local, page_length, head_dim
    )
    new_values = jnp.where(live_child, landed_values, zero).reshape(
        local_beams * pages, kv_local, page_length, head_dim
    )
    return (attention, step_score, child_score, new_keys, new_values)


def per_device(*args):
    (queries, fresh_keys, fresh_values, key_pool, value_pool, page_table) = args[:6]
    (lengths, score_weight, running_min, boundary, parents, homes) = args[6:]
    local = queries.shape[0]
    pool, kv, page, head_dim = key_pool.shape
    tables, need = plan(parents, homes, lengths, page_table)

    def streamed(z_slots, y_slots, d_slots):
        attention, score, new_keys, new_values = move(
            z_slots,
            y_slots,
            d_slots,
            tables,
            running_min,
            boundary,
            fresh_keys,
            fresh_values,
            queries.reshape(local, -1, head_dim),
            score_weight.reshape(-1, head_dim),
            key_pool.reshape(pool, page, head_dim),
            value_pool.reshape(pool, page, head_dim),
        )
        return (
            attention.reshape(queries.shape),
            score[0, :local],
            score[1, :local],
            new_keys.reshape(key_pool.shape),
            new_values.reshape(value_pool.shape),
        )

    ways = [functools.partial(streamed, *r) for r in ROUTES]
    return lax.switch(need[0], ways + [lambda: whole_exchange(*args)])


def solution(mesh):
    in_specs = (
        P("beam", "mp"),
        P("beam", "mp"),
        P("beam", "mp"),
        P("beam", "mp", None, None),
        P("beam", "mp", None, None),
        P("beam", None),
        P(),
        P("mp"),
        P("beam"),
        P("beam"),
        P(),
        P(),
    )
    out_specs = (
        P("beam", "mp"),
        P("beam"),
        P("beam"),
        P("beam", "mp", None, None),
        P("beam", "mp", None, None),
    )
    return jax.shard_map(
        per_device, mesh=mesh, in_specs=in_specs, out_specs=out_specs, check_vma=False
    )
```

```python
import functools
import math

import jax
import jax.numpy as jnp
from jax import lax
from jax.experimental import pallas as pl
from jax.experimental.pallas import tpu as pltpu
from jax.sharding import PartitionSpec as P

WAIT = 4
Y_WAIT = 3
Z_BUFS = 8
Y_BUFS = 4
RING_Z = 8
RING_Y = 4
ROUTES = ((72, 38, 36), (80, 44, 40))
ROUNDS = 2
CHUNK = 64
LOADS = 4
VMEM_BYTES = 49 * 1024 * 1024
PAGE = 128
LANES = 128
Z_ROW, Y_ROW, STORE_ROW, LAND_ROW, MOVED_ROW = 0, 2, 5, 6, 7
FRESH_ROW, WHO_ROW, PARENT_ROW, LENGTH_ROW, OWN_ROW = 8, 9, 10, 11, 12
PAGE_ROW = 13
MESH = pl.DeviceIdType.MESH


def planning(parents_ref, homes_ref, lengths_ref, table_ref, tab_ref, need_ref):
    f32 = jnp.float32
    beams = parents_ref.shape[1]
    local, pages = table_ref.shape
    pool = local * pages
    rank = lax.axis_index("beam")
    rank_f = rank.astype(f32)
    row_f, col_f = (rank // RING_Z).astype(f32), (rank % RING_Z).astype(f32)

    def iota(shape, dim):
        return lax.broadcasted_iota(jnp.int32, shape, dim).astype(f32)

    def div(x, n):
        return jnp.floor(x * (1.0 / n))

    def mod(x, n):
        return x - n * div(x, n)

    def columns(*rows):
        packed = jnp.concatenate(
            list(rows) + [jnp.zeros((8 - len(rows), beams), f32)] * (len(rows) < 8), axis=0
        )
        turned = jnp.transpose(packed)
        return [turned[:, i : i + 1] for i in range(len(rows))]

    def add(mask, column):
        return jnp.sum(jnp.where(mask, column, 0.0), axis=0, keepdims=True)

    def sweep(terms, greatest=False):
        fold, total = (jnp.maximum, jnp.max) if greatest else (jnp.add, jnp.sum)
        held = None
        for i in range(0, beams, CHUNK):
            parts = [
                total(x.reshape(CHUNK // 8, 8, x.shape[1]), axis=0)
                for x in terms(slice(i, i + CHUNK))
            ]
            held = parts if held is None else [fold(x, y) for x, y in zip(held, parts)]
        return [total(x, axis=0, keepdims=True) for x in held]

    def when(mask, column):
        return jnp.where(mask, column, 0.0)

    parents, homes, lengths = (
        ref[...].astype(f32) for ref in (parents_ref, homes_ref, lengths_ref)
    )
    parents_c, homes_c, lengths_c = columns(parents, homes, lengths)
    every = iota((1, beams), 1)
    every_c = iota((beams, 1), 0)
    (q,) = sweep(lambda r: [when(homes_c[r] == every, parents_c[r])])
    (length,) = sweep(lambda r: [when(every_c[r] == q, lengths_c[r])])
    up = div(length, PAGE) + 1.0
    src, dst = div(q, local), div(every, local)
    sy, sz, dy, dz = div(src, RING_Z), mod(src, RING_Z), div(dst, RING_Z), mod(dst, RING_Z)
    d = mod(dz - sz + RING_Z, RING_Z)
    turn = mod(dy - sy + RING_Y, RING_Y)
    near_p, near_m = when(d < 4, d), when(d > 4, RING_Z - d)
    near_4 = when(d == 4, 1.0)
    kind = jnp.where(turn == 2, 2.0, jnp.where(turn == 0, 0.0, 1.0))
    q_c, up_c, d_c, src_c, near_p_c, near_m_c, near_4_c, kind_c = columns(
        q, up, d, src, near_p, near_m, near_4, kind
    )

    def siblings(r):
        sib = q_c[r] == q
        held = [when(sib, x[r]) for x in (near_p_c, near_m_c, near_4_c)]
        return held + [when(sib, every - every_c[r])]

    far_p, far_m, far_4, since = sweep(siblings, True)
    far_4, first = far_4 > 0, since == 0
    plus4 = far_4 & ((far_p > far_m) | ((far_p == far_m) & (mod(q, 2) == 1)))
    up_first = jnp.where(first, up, 0.0)
    lane = iota((1, LANES), 1)
    at_z = mod(lane, RING_Z)
    from_node = jnp.where(src_c == lane, 1.0, 0.0)
    at_node = jnp.where(iota((LANES, 1), 0) == src, 1.0, 0.0)

    def back(x, n):
        n = n % RING_Z
        if n == 0:
            return x
        full = jnp.broadcast_to(x, (8, LANES))
        near = pltpu.roll(full, n, 1)
        wrap = pltpu.roll(full, LANES + n - RING_Z, 1)
        return jnp.where(at_z >= n, near, wrap)[:1]

    def reach(plus):
        plus = jnp.where(plus, 1.0, 0.0)
        split = jnp.where(far_4, 1.0, 0.0)
        a = jnp.maximum(far_p, 4.0 * split * plus)
        b = jnp.maximum(far_m, 4.0 * split * (1.0 - plus))
        weights = jnp.concatenate(
            [jnp.where(far >= j, up_first, 0.0) for far in (a, b) for j in range(1, 5)], axis=0
        )
        count = jnp.dot(weights, from_node, preferred_element_type=f32)
        held = [
            [back(count[4 * n + j : 4 * n + j + 1], (1 - 2 * n) * j) for j in range(4)]
            for n in range(2)
        ]
        return a, b, held

    for turn_now in range(ROUNDS):
        a, b, helds = reach(plus4)
        loads = [sum(held) for held in helds]
        ahead = [back(loads[n], (2 * n - 1) * j) for n in range(2) for j in range(4)]
        seen = jnp.dot(jnp.concatenate(ahead, axis=0), at_node, preferred_element_type=f32)
        plus = jnp.where(plus4, 1.0, 0.0)
        cost_p, cost_m = jnp.zeros((1, beams), f32), jnp.zeros((1, beams), f32)
        for j in range(4):
            over_p = jnp.maximum(seen[j : j + 1] + up * (1 - plus) - 30, 0.0)
            over_m = jnp.maximum(seen[4 + j : 5 + j] + up * plus - 30, 0.0)
            cost_p += jnp.where(far_p <= j, over_p * over_p, 0.0)
            cost_m += jnp.where(far_m <= j, over_m * over_m, 0.0)
        moves = mod(q + src, ROUNDS) == turn_now
        want = jnp.where(cost_p < cost_m, 1.0, 0.0)
        plus4 = jnp.where(moves, want, plus) > 0
    a, b, helds = reach(plus4)
    goes_p = (d > 0) & ((d < 4) | ((d == 4) & (a == 4)))
    k = jnp.where(goes_p, d, mod(RING_Z - d, RING_Z))
    def last_kind(r):
        sib = q_c[r] == q
        at_p, at_m = sib & (d_c[r] == a), sib & (d_c[r] == RING_Z - b)
        return [when(at_p, kind_c[r]), when(at_m, kind_c[r])]

    kinds = sweep(last_kind, True)
    keys = [(4 * x + y) * beams + beams - 1 - q for x, y in zip((a, b), kinds)]
    ups = [when(x > 0, up_first) for x in (a, b)]
    keys_c, ups_c = [None] * 2, [None] * 2
    keys_c[0], keys_c[1], ups_c[0], ups_c[1] = columns(*keys, *ups)

    def ahead_of(r):
        same = src_c[r] == src
        return [when(same & (keys_c[n][r] > keys[n]), ups_c[n][r]) for n in range(2)]

    pos_p, pos_m = sweep(ahead_of)

    starts, total = [], jnp.zeros((1, LANES), f32)
    for side in range(2):
        step = 1 - 2 * side
        held = helds[side]
        start = [jnp.zeros((1, LANES), f32)]
        for j in range(1, 4):
            start.append(jnp.maximum(start[-1] + held[j - 1], back(start[-1], step) + WAIT))
        for j in range(4):
            total = jnp.maximum(total, jnp.where(held[j] > 0, start[j] + held[j], 0.0))
        starts.append(start)
    z_total = jnp.max(total)
    node = sy * RING_Z + mod(jnp.where(goes_p, dz + RING_Z - 1, dz + 1), RING_Z)
    spots = jnp.where(iota((LANES, 1), 0) == node, 1.0, 0.0)
    seen = jnp.dot(
        jnp.concatenate(starts[0] + starts[1], axis=0), spots,
        preferred_element_type=f32, precision=lax.Precision.HIGHEST,
    )
    seen = jnp.floor(seen + 0.5)
    cell = jnp.where(goes_p, 0.0, 4.0) + k - 1
    arrive = jnp.zeros((1, beams), f32)
    for j in range(8):
        arrive = jnp.where(cell == j, seen[j : j + 1], arrive)
    arrive = jnp.where(d == 0, -1.0 * WAIT, arrive + jnp.where(goes_p, pos_p, pos_m))
    ready = div(arrive + WAIT, 2)
    queue = jnp.where(turn > 0, (sy * RING_Z + dz) * RING_Y + turn, -1 - every)
    rank_key = ready * beams + every
    queue_c, rank_c = columns(queue, rank_key)
    (queued,) = sweep(
        lambda r: [when((queue_c[r] == queue) & (rank_c[r] < rank_key), up_c[r])]
    )
    (late_c,) = columns(ready - queued + beams)
    (late,) = sweep(
        lambda r: [when((queue_c[r] == queue) & (rank_c[r] <= rank_key), late_c[r])], True
    )
    slot = queued + late - beams
    ends = slot + up
    a_total = jnp.max(jnp.where((turn == 1) | (turn == 3), ends, 0.0))
    d_total = jnp.max(jnp.where(turn == 2, ends, 0.0))
    route = jnp.float32(len(ROUTES))
    for n in reversed(range(len(ROUTES))):
        z_slots, y_slots, d_slots = ROUTES[n]
        fits = (z_total <= z_slots) & (a_total <= y_slots) & (d_total <= d_slots)
        route = jnp.where(fits, jnp.float32(n), route)
    need_ref[0] = route.astype(jnp.int32)

    table = table_ref[...].astype(f32)
    mine = jnp.where(iota((local, 1), 0) + rank_f * local == q, 1.0, 0.0)
    own_page = lax.dot_general(
        table, mine, (((0,), (0,)), ((), ())), preferred_element_type=f32
    )
    own = [own_page[p : p + 1] for p in range(pages)]
    target = iota((LANES, 1), 0)

    def line(spots, values):
        held = sum(when(spot == target, value) for spot, value in zip(spots, values))
        held = sum(held[:, n : n + LANES] for n in range(0, beams, LANES))
        return jnp.sum(jnp.transpose(held), axis=0, keepdims=True)

    def spread(mask, at):
        return [jnp.where(mask & (up > p), at + p, -1.0) for p in range(pages)]

    tables = [
        line(spread((src == rank_f) & first & (far > 0), pos), own)
        for far, pos in ((a, pos_p), (b, pos_m))
    ]
    base = jnp.where(goes_p, pool * 1.0, pool + 1.0) + 2 * arrive
    held_at = [jnp.where(d == 0, own[p], base + 2 * p) for p in range(pages)]
    at_me = (sy == row_f) & (dz == col_f)
    for way in (1.0, 3.0, 2.0):
        tables.append(line(spread(at_me & (turn == way), slot), held_at))
    way_of = jnp.where(turn == 1, 0.0, jnp.where(turn == 3, 1.0, 2.0))
    child = every - rank_f * local
    is_mine = (child >= 0) & (child < local)
    tables.append(line(spread(is_mine & (turn == 0), pages * child), held_at))
    lands = line(
        spread(is_mine & (turn > 0), pages * child),
        [3 * (slot + p) + way_of + 1 for p in range(pages)],
    )
    tables += [jnp.maximum(lands - 1, 0.0), when(lands > 0, 1.0)]
    for side in range(2):
        step = 1 - 2 * side
        for j in range(1, 4):
            pick = lambda x: jnp.sum(jnp.where(lane == rank_f, x, 0.0), axis=1, keepdims=True)
            lo, n = pick(starts[side][j]), pick(helds[side][j])
            was = pick(back(starts[side][j - 1], step))
            tables[side] = jnp.where(
                (lane >= lo) & (lane < lo + n), pool + side + 2 * (lane - lo + was), tables[side]
            )
    owner = rank_f * local + iota((local, 1), 0)
    own_len = jnp.sum(jnp.where(every == owner, lengths, 0.0), axis=1, keepdims=True)
    fresh, who = jnp.zeros((1, LANES), f32), jnp.zeros((1, LANES), f32)
    for p in range(pages):
        hit = (table[:, p : p + 1] == lane) & (div(own_len, PAGE) == p)
        fresh += add(hit, mod(own_len, PAGE) + 1)
        who += add(hit, iota((local, 1), 0))
    tables += [fresh - 1, who]
    own_lane = jnp.where(is_mine, child, -1.0)
    tables += [line([own_lane], [x]) for x in (q, length, lengths)]
    at_beam = iota((local, 1), 0) == div(lane, pages)
    tables.append(
        sum(add(at_beam & (mod(lane, pages) == p), table[:, p : p + 1]) for p in range(pages))
    )
    tables += [jnp.zeros((1, LANES), f32)] * (16 - len(tables))
    tab_ref[...] = jnp.concatenate(tables, axis=0).astype(jnp.int32)


def plan(parents, homes, lengths, page_table):
    vmem = pl.BlockSpec(memory_space=pltpu.VMEM)
    return pl.pallas_call(
        planning,
        out_shape=(
            jax.ShapeDtypeStruct((16, LANES), jnp.int32),
            jax.ShapeDtypeStruct((1,), jnp.int32),
        ),
        in_specs=[vmem] * 4,
        out_specs=(vmem, pl.BlockSpec(memory_space=pltpu.SMEM)),
        name="plan_moves",
    )(parents[None], homes[None], lengths[None], page_table)


def moving(z_slots, y_slots, d_slots, *refs):
    tab, least, ends, fk, fv, q_ref, sw, kp, vp, att, score, nk, nv = refs[:13]
    store, land_z, land_y, relay, buf_z, buf_y, sums, land_s, land_u, fresh, raw = refs[13:24]
    send_z, recv_z, send_y, recv_y, recv_r, send_r, send_s, recv_s, send_u, recv_u, send_l = refs[24:]
    pool = kp.shape[0]
    local, heads, head_dim = q_ref.shape
    pages = pool // local
    f32 = jnp.float32
    me, part = lax.axis_index("beam"), lax.axis_index("mp")
    parts = lax.axis_size("mp")
    row, col = me // RING_Z, me % RING_Z

    def at_z(n):
        return row * RING_Z + lax.rem(col + n, RING_Z)

    def at_y(n):
        return lax.rem(row + n, RING_Y) * RING_Z + col

    z_to, y_to = (at_z(1), at_z(RING_Z - 1)), (at_y(1), at_y(RING_Y - 1))
    barrier = pltpu.get_barrier_semaphore()

    share = pool // LOADS

    def load(half, n):
        part_of = pl.ds(n * share, share)
        return pltpu.make_async_copy(
            (kp, vp)[half].at[part_of], raw.at[half, part_of], send_l.at[half * LOADS + n]
        )

    for n in range(LOADS):
        load(0, n).start()
        load(1, n).start()

    def greet(where):
        pl.semaphore_signal(barrier, inc=1, device_id=where, device_id_type=MESH)

    for n in range(1, RING_Z):
        greet({"beam": at_z(n)})
    for n in range(1, RING_Y):
        greet({"beam": at_y(n)})
    for n in range(1, parts):
        greet({"mp": lax.rem(part + n, parts)})

    rows = lax.broadcasted_iota(jnp.int32, (PAGE, head_dim), 0)
    for n, new in enumerate((fk, fv)):
        lines = new[...].astype(f32)
        for i in range(local):
            fresh[n, i] = lines[i : i + 1]

    def fill(i, carry):
        hit = rows == tab[FRESH_ROW, i]
        who = tab[WHO_ROW, i]
        for half in range(2):
            line = jnp.broadcast_to(fresh[half, who], (PAGE, head_dim))
            page = jnp.where(hit, line, raw[half, i].astype(f32))
            store[i, half * PAGE : half * PAGE + PAGE] = page.astype(jnp.bfloat16)
        return carry

    for n in range(LOADS):
        load(0, n).wait()
        load(1, n).wait()
        lax.fori_loop(n * share, n * share + share, fill, 0, unroll=4)
    pl.semaphore_wait(barrier, RING_Z + RING_Y + parts - 3)

    def remote(source, target, sent, got, where):
        return pltpu.make_async_remote_copy(
            source, target, sent, got, device_id=where, device_id_type=MESH
        )

    def z_copy(side, t, b):
        b = side * Z_BUFS + b
        return remote(
            buf_z.at[b], land_z.at[2 * t + side], send_z.at[b], recv_z.at[2 * t + side],
            {"beam": z_to[side]},
        )

    def a_copy(side, s, b):
        b = side * Y_BUFS + b
        return remote(
            buf_y.at[b], land_y.at[3 * s + side], send_y.at[b], recv_y.at[3 * s + side],
            {"beam": y_to[side]},
        )

    def d_copy(side, s, b):
        b = 2 * Y_BUFS + b
        return remote(buf_y.at[b], relay.at[s], send_y.at[b], recv_r.at[s], {"beam": y_to[side]})

    def r_copy(side, s):
        return remote(
            relay.at[s], land_y.at[3 * s + 2], send_r.at[s], recv_y.at[3 * s + 2],
            {"beam": y_to[side]},
        )

    def s_copy(n, origin):
        return remote(
            sums, land_s.at[origin], send_s.at[n], recv_s.at[origin],
            {"mp": lax.rem(part + n, parts)},
        )

    def u_copy(n, origin):
        spot = land_u.at[row, origin]
        return remote(spot, spot, send_u.at[n], recv_u.at[origin], {"beam": at_z(n)})

    def v_copy(n, origin):
        spot = land_u.at[origin]
        return remote(
            spot, spot, send_u.at[RING_Z + n], recv_u.at[RING_Z + origin], {"beam": at_y(n)}
        )

    def z_slot(g, j):
        t = 4 * g + j

        @pl.when((t >= WAIT) & (t < z_slots + WAIT))
        def _():
            for side in range(2):
                z_copy(side, t - WAIT, 0).wait_recv()
                at = 2 * (t - WAIT) + side
                store[pool + at] = land_z[at]

        @pl.when(t < z_slots)
        def _():
            b = lax.rem(g, 2) * 4 + j
            for side in range(2):

                @pl.when(g >= 2)
                def _(side=side):
                    z_copy(side, t - Z_BUFS, b).wait_send()

                buf_z[side * Z_BUFS + b] = store[tab[Z_ROW + side, t]]
                z_copy(side, t, b).start()

    def y_slot(g, j):
        s = 2 * g + j

        @pl.when(s < d_slots)
        def _():
            b = lax.rem(g, 2) * 2 + j

            @pl.when(g >= 2)
            def _():
                d_copy(j, s - Y_BUFS, b).wait_send()

            buf_y[2 * Y_BUFS + b] = store[tab[Y_ROW + 2, s]]
            d_copy(j, s, b).start()

        @pl.when(s < y_slots)
        def _():
            b = lax.rem(g, 2) * 2 + j

            @pl.when(g >= 2)
            def _():
                a_copy(0, s - Y_BUFS, b).wait_send()
                a_copy(1, s - Y_BUFS, b).wait_send()

            for way in range(2):
                buf_y[way * Y_BUFS + b] = store[tab[Y_ROW + way, s]]
            a_copy(0, s, b).start()
            a_copy(1, s, b).start()

        @pl.when((s >= Y_WAIT) & (s < d_slots + Y_WAIT))
        def _():
            side = 1 - j if Y_WAIT % 2 else j
            d_copy(side, s - Y_WAIT, 0).wait_recv()
            r_copy(side, s - Y_WAIT).start()

    def attend(i):
        keys = jnp.concatenate([store[tab[PAGE_ROW, pages * i + p], :PAGE] for p in range(pages)], axis=0)
        logits = lax.dot_general(
            q_ref[i], keys, (((1,), (1,)), ((), ())), preferred_element_type=f32
        ) * (1.0 / math.sqrt(head_dim))
        token = lax.broadcasted_iota(jnp.int32, logits.shape, 1)
        logits = jnp.where(token <= tab[OWN_ROW, i], logits, -jnp.inf)
        powers = jnp.exp(logits - jnp.max(logits, axis=1, keepdims=True))
        weights = (powers / jnp.sum(powers, axis=1, keepdims=True)).astype(jnp.bfloat16)
        values = jnp.concatenate([store[tab[PAGE_ROW, pages * i + p], PAGE:] for p in range(pages)], axis=0)
        mixed = jnp.dot(weights, values, preferred_element_type=f32).astype(jnp.bfloat16)
        att[i] = mixed
        mixed = mixed.astype(f32)
        for n, other in enumerate((mixed, sw[...].astype(f32))):
            total = jnp.sum(jnp.sum(mixed * other, axis=1, keepdims=True), axis=0, keepdims=True)
            sums[n, i] = jnp.broadcast_to(total, (1, LANES))

    lane = lax.broadcasted_iota(jnp.int32, (1, LANES), 1)

    def tell_sums():
        land_s[part] = sums[...]
        for n in range(1, parts):
            s_copy(n, part).start()

    def tell_updated():
        for n in range(1, parts):
            s_copy(n, lax.rem(part + parts - n, parts)).wait_recv()
        both = land_s[0]
        for n in range(1, parts):
            both += land_s[n]
        updated = jnp.zeros((1, LANES), f32)
        steps = jnp.zeros((1, LANES), f32)
        for i in range(local):
            width = heads * head_dim * parts
            step = jax.nn.sigmoid(both[1, i] * lax.rsqrt(both[0, i] / width + 1e-06))
            floor = jnp.broadcast_to(least[i], (1, LANES))
            ended = jnp.broadcast_to(ends[i], (1, LANES)) == 1
            new = jnp.where(ended, jnp.minimum(floor, step), floor)
            steps = jnp.where(lane == i, step, steps)
            updated = jnp.where(lane == i, new, updated)
        score[0:1, :] = steps
        land_u[row, col] = updated
        for n in range(1, RING_Z):
            u_copy(n, col).start()

    def tell_row():
        for n in range(1, RING_Z):
            u_copy(n, lax.rem(col + RING_Z - n, RING_Z)).wait_recv()
        for n in range(1, RING_Y):
            v_copy(n, row).start()

    def give_children():
        for n in range(1, RING_Y):
            v_copy(n, lax.rem(row + RING_Y - n, RING_Y)).wait_recv()
        out = jnp.zeros((1, LANES), f32)
        for i in range(local):
            q = tab[PARENT_ROW, i]
            line = land_u[q // (local * RING_Z), (q // local) % RING_Z]
            value = jnp.sum(jnp.where(lane == q % local, line, 0.0), axis=1, keepdims=True)
            out = jnp.where(lane == i, jnp.broadcast_to(value, (1, LANES)), out)
        score[1:2, :] = out
        for n in range(1, parts):
            s_copy(n, part).wait_send()
        for n in range(1, RING_Z):
            u_copy(n, col).wait_send()
        for n in range(1, RING_Y):
            v_copy(n, row).wait_send()

    def group(g, carry):
        z_slot(g, 0)
        z_slot(g, 1)
        y_slot(g, 0)

        @pl.when(g < local)
        def _():
            attend(g)

        z_slot(g, 2)
        z_slot(g, 3)
        y_slot(g, 1)
        for n, act in enumerate((tell_sums, tell_updated, tell_row, give_children)):
            pl.when(g == local + (0, 1, 2, 3)[n])(act)
        return carry

    groups = max(-(-(z_slots + WAIT) // 4), -(-max(y_slots, d_slots + Y_WAIT) // 2))
    lax.fori_loop(0, groups, group, 0)

    def drain(i, carry):
        for j in range(2):
            s = 2 * i + j
            a_copy(0, s, 0).wait_recv()
            a_copy(1, s, 0).wait_recv()
        return carry

    def drain_d(i, carry):
        for j in range(2):
            s = 2 * i + j
            r_copy(j, s).wait_recv()
            r_copy(j, s).wait_send()
        return carry

    lax.fori_loop(0, y_slots // 2, drain, 0)
    lax.fori_loop(0, d_slots // 2, drain_d, 0)
    for b in range(Z_BUFS):
        for side in range(2):
            z_copy(side, 0, b).wait_send()
    for b in range(Y_BUFS):
        a_copy(0, 0, b).wait_send()
        a_copy(1, 0, b).wait_send()
        d_copy(b % 2, 0, b).wait_send()

    def finish(i, carry):
        moved = jnp.broadcast_to(tab[MOVED_ROW, i], (PAGE, head_dim)) > 0
        live = rows + lax.rem(i, pages) * PAGE <= tab[LENGTH_ROW, i // pages]
        for half, out in enumerate((nk, nv)):
            side = pl.ds(half * PAGE, PAGE)
            here = store[tab[STORE_ROW, i], side].astype(f32)
            there = land_y[tab[LAND_ROW, i], side].astype(f32)
            page = jnp.where(live, jnp.where(moved, there, here), 0.0)
            out[i] = page.astype(jnp.bfloat16)
        return carry

    lax.fori_loop(0, pool, finish, 0, unroll=4)


def move(z_slots, y_slots, d_slots, tables, running_min, boundary, fresh_k, fresh_v, query,
         score_weight, keys, values):
    pool = keys.shape[0]
    page = (2 * PAGE, keys.shape[2])
    out = jax.ShapeDtypeStruct(keys.shape, keys.dtype)
    vmem, smem = pl.BlockSpec(memory_space=pltpu.VMEM), pl.BlockSpec(memory_space=pltpu.SMEM)
    dma = pltpu.SemaphoreType.DMA
    parts = lax.axis_size("mp")
    local = query.shape[0]
    return pl.pallas_call(
        functools.partial(moving, z_slots, y_slots, d_slots),
        out_shape=(
            jax.ShapeDtypeStruct(query.shape, query.dtype),
            jax.ShapeDtypeStruct((2, LANES), jnp.float32),
            out,
            out,
        ),
        in_specs=[smem] * 3 + [vmem] * 4 + [pl.BlockSpec(memory_space=pl.ANY)] * 2,
        out_specs=(vmem,) * 4,
        scratch_shapes=[
            pltpu.VMEM((pool + 2 * z_slots, *page), jnp.bfloat16),
            pltpu.VMEM((2 * z_slots, *page), jnp.bfloat16),
            pltpu.VMEM((3 * y_slots, *page), jnp.bfloat16),
            pltpu.VMEM((d_slots, *page), jnp.bfloat16),
            pltpu.VMEM((2 * Z_BUFS, *page), jnp.bfloat16),
            pltpu.VMEM((3 * Y_BUFS, *page), jnp.bfloat16),
            pltpu.VMEM((2, local, 1, LANES), jnp.float32),
            pltpu.VMEM((parts, 2, local, 1, LANES), jnp.float32),
            pltpu.VMEM((RING_Y, RING_Z, 1, LANES), jnp.float32),
            pltpu.VMEM((2, local, 1, keys.shape[2]), jnp.float32),
            pltpu.VMEM((2, *keys.shape), jnp.bfloat16),
            dma((2 * Z_BUFS,)),
            dma((2 * z_slots,)),
            dma((3 * Y_BUFS,)),
            dma((3 * y_slots,)),
            dma((d_slots,)),
            dma((d_slots,)),
            dma((parts,)),
            dma((parts,)),
            dma((RING_Z + RING_Y,)),
            dma((RING_Z + RING_Y,)),
            dma((2 * LOADS,)),
        ],
        compiler_params=pltpu.CompilerParams(
            collective_id=ROUTES.index((z_slots, y_slots, d_slots)),
            has_side_effects=True,
            vmem_limit_bytes=VMEM_BYTES,
        ),
        name="move_pages",
    )(tables, running_min, boundary, fresh_k, fresh_v, query, score_weight, keys, values)


def sent_to_all(array, axis):
    copies = jnp.broadcast_to(array, (lax.axis_size(axis), *array.shape))
    return lax.all_to_all(copies, axis, split_axis=0, concat_axis=0, tiled=True)


def over_copies(array, axis):
    return sent_to_all(array, axis).sum(axis=0)


def packed_total(arrays, axis):
    ends = [0]
    for a in arrays:
        ends.append(ends[-1] + a.size)
    running = over_copies(jnp.concatenate([a.ravel() for a in arrays]), axis)
    return tuple((running[b:e].reshape(a.shape) for a, b, e in zip(arrays, ends, ends[1:])))


def laid_out(parts, dim):
    parts = jnp.moveaxis(parts, 0, dim)
    dims = parts.shape
    return parts.reshape(*dims[:dim], dims[dim] * dims[dim + 1], *dims[dim + 2 :])


def collect(array, axis, dim):
    return laid_out(sent_to_all(array, axis), dim)


def whole_exchange(
    queries,
    fresh_keys,
    fresh_values,
    key_pool,
    value_pool,
    page_table,
    lengths,
    score_weight,
    running_min,
    boundary,
    parents,
    homes,
):
    ranks = lax.axis_size("beam")
    rank = lax.axis_index("beam")
    local_beams, pages = page_table.shape
    kv_local = key_pool.shape[1]
    page_length = key_pool.shape[2]
    head_dim = key_pool.shape[3]
    heads_local = queries.shape[1] // head_dim
    group = heads_local // kv_local
    beams = lengths.shape[0]
    capacity = (local_beams + ranks - 1) // ranks
    slot_cap = capacity * pages
    buffer_rows = ranks * slot_cap
    everyone = jnp.arange(beams, dtype=jnp.int32)
    page_ids = jnp.arange(pages, dtype=jnp.int32)
    token_grid = page_ids[:, None] * page_length + jnp.arange(page_length, dtype=jnp.int32)[None, :]
    parent_hit = parents[:, None] == everyone[None, :]
    parent_len = jnp.sum(jnp.where(parent_hit, lengths[None, :], 0), axis=1)
    used_pages = parent_len // page_length + 1
    source = parents // local_beams
    destination = homes // local_beams
    earlier = everyone[None, :] < everyone[:, None]
    same_pair = (
        (source[:, None] == source[None, :])
        & (destination[:, None] == destination[None, :])
        & earlier
    )
    offset_table = jnp.sum(jnp.where(same_pair, used_pages[None, :], 0), axis=1)
    sending = (source == rank)[:, None] & (page_ids[None, :] < used_pages[:, None])
    dest_rows = destination[:, None] * slot_cap + offset_table[:, None] + page_ids[None, :]
    dest_rows = jnp.where(sending, dest_rows, buffer_rows)
    local_parent = jnp.clip(parents - rank * local_beams, 0, local_beams - 1)
    source_slots = page_table[local_parent]
    send_table = (
        jnp.zeros((buffer_rows,), jnp.int32)
        .at[dest_rows.reshape(-1)]
        .set(source_slots.reshape(-1), mode="drop")
    )
    positions = rank * local_beams + jnp.arange(local_beams, dtype=jnp.int32)
    child_hit = homes[None, :] == positions[:, None]
    child_source = jnp.sum(jnp.where(child_hit, source[None, :], 0), axis=1)
    child_offset = jnp.sum(jnp.where(child_hit, offset_table[None, :], 0), axis=1)
    child_len = jnp.sum(jnp.where(child_hit, parent_len[None, :], 0), axis=1)
    child_parent = jnp.sum(jnp.where(child_hit, parents[None, :], 0), axis=1)
    recv_rows = jnp.clip(
        child_source[:, None] * slot_cap + child_offset[:, None] + page_ids[None, :],
        0,
        buffer_rows - 1,
    )
    own_len = lax.dynamic_slice_in_dim(lengths, rank * local_beams, local_beams)
    last_page = jnp.take_along_axis(page_table, (own_len // page_length)[:, None], axis=1)[:, 0]
    offset_in = own_len % page_length
    slot_ids = jnp.arange(key_pool.shape[0], dtype=jnp.int32)
    hit = last_page[None, :] == slot_ids[:, None]
    writer = jnp.sum(jnp.where(hit, jnp.arange(local_beams, dtype=jnp.int32), 0), axis=1)
    at = jnp.sum(jnp.where(hit, offset_in[None, :] + 1, 0), axis=1) - 1
    written = (at[:, None] == jnp.arange(page_length, dtype=jnp.int32))[:, None, :, None]

    def with_fresh(fresh, old):
        rows = fresh.reshape(local_beams, kv_local, 1, head_dim)[writer]
        return jnp.where(written, rows, old)

    keys_now = with_fresh(fresh_keys, key_pool)
    values_now = with_fresh(fresh_values, value_pool)
    scale = 1.0 / math.sqrt(head_dim)
    key_rows = keys_now[page_table]
    value_rows = values_now[page_table]
    query = queries.reshape(local_beams, kv_local, group, head_dim)
    scores = (
        jnp.einsum("bhgd,bphtd->bhgpt", query, key_rows, preferred_element_type=jnp.float32) * scale
    )
    live_own = (token_grid[None] <= own_len[:, None, None])[:, None, None]
    scores = jnp.where(live_own, scores, -jnp.inf)
    flattened_scores = scores.reshape(local_beams, kv_local, group, pages * page_length)
    weights = jax.nn.softmax(flattened_scores, axis=-1).astype(jnp.bfloat16).reshape(scores.shape)
    mixed = jnp.einsum("bhgpt,bphtd->bhgd", weights, value_rows, preferred_element_type=jnp.float32)
    attention = mixed.reshape(local_beams, heads_local * head_dim).astype(jnp.bfloat16)
    as_float = attention.astype(jnp.float32)
    partial_square = jnp.sum(as_float * as_float, axis=1)
    partial_dot = jnp.sum(as_float * score_weight.astype(jnp.float32)[None, :], axis=1)
    total_square, total_dot = packed_total((partial_square, partial_dot), "mp")
    width = heads_local * head_dim * lax.axis_size("mp")
    step_score = jax.nn.sigmoid(total_dot * lax.rsqrt(total_square / width + 1e-06))
    updated = jnp.where(boundary == 1, jnp.minimum(running_min, step_score), running_min)
    every_updated = collect(updated, "beam", 0)
    child_score = jnp.sum(
        jnp.where(child_parent[:, None] == everyone[None, :], every_updated[None, :], 0.0), axis=1
    )
    moved_keys, moved_values = (
        lax.all_to_all(keys_now[send_table], "beam", split_axis=0, concat_axis=0, tiled=True),
        lax.all_to_all(values_now[send_table], "beam", split_axis=0, concat_axis=0, tiled=True),
    )
    landed_keys = moved_keys[recv_rows]
    landed_values = moved_values[recv_rows]
    live_child = (token_grid[None] <= child_len[:, None, None])[:, :, None, :, None]
    zero = jnp.zeros((), landed_keys.dtype)
    new_keys = jnp.where(live_child, landed_keys, zero).reshape(
        local_beams * pages, kv_local, page_length, head_dim
    )
    new_values = jnp.where(live_child, landed_values, zero).reshape(
        local_beams * pages, kv_local, page_length, head_dim
    )
    return (attention, step_score, child_score, new_keys, new_values)


def per_device(*args):
    (queries, fresh_keys, fresh_values, key_pool, value_pool, page_table) = args[:6]
    (lengths, score_weight, running_min, boundary, parents, homes) = args[6:]
    local = queries.shape[0]
    pool, kv, page, head_dim = key_pool.shape
    tables, need = plan(parents, homes, lengths, page_table)

    def streamed(z_slots, y_slots, d_slots):
        attention, score, new_keys, new_values = move(
            z_slots,
            y_slots,
            d_slots,
            tables,
            running_min,
            boundary,
            fresh_keys,
            fresh_values,
            queries.reshape(local, -1, head_dim),
            score_weight.reshape(-1, head_dim),
            key_pool.reshape(pool, page, head_dim),
            value_pool.reshape(pool, page, head_dim),
        )
        return (
            attention.reshape(queries.shape),
            score[0, :local],
            score[1, :local],
            new_keys.reshape(key_pool.shape),
            new_values.reshape(value_pool.shape),
        )

    ways = [functools.partial(streamed, *r) for r in ROUTES]
    return lax.switch(need[0], ways + [lambda: whole_exchange(*args)])


def solution(mesh):
    in_specs = (
        P("beam", "mp"),
        P("beam", "mp"),
        P("beam", "mp"),
        P("beam", "mp", None, None),
        P("beam", "mp", None, None),
        P("beam", None),
        P(),
        P("mp"),
        P("beam"),
        P("beam"),
        P(),
        P(),
    )
    out_specs = (
        P("beam", "mp"),
        P("beam"),
        P("beam"),
        P("beam", "mp", None, None),
        P("beam", "mp", None, None),
    )
    return jax.shard_map(
        per_device, mesh=mesh, in_specs=in_specs, out_specs=out_specs, check_vma=False
    )
```
